8 devices in a mesh: sp: 8 (over z, y, x, core).
Axes of the slice: x: 2, y: 2, z: 1, core: 2. Of those that a mesh axis runs over, the one named last changes fastest.
Arguments:
- hidden: bfloat16 [16, 1024, 2048], P(None, 'sp')
- d_out: bfloat16 [16, 1024, 2048], P(None, 'sp')
- w_query: bfloat16 [2048, 8, 256], replicated
- w_key: bfloat16 [2048, 256], replicated
- w_value: bfloat16 [2048, 256], replicated
- w_out: bfloat16 [8, 256, 2048], replicated
Outputs:
- output 1: bfloat16 [16, 1024, 2048], P(None, 'sp')
- output 2: bfloat16 [16, 1024, 2048], P(None, 'sp')
- output 3: float32 [2048, 8, 256], replicated
- output 4: float32 [2048, 256], replicated
- output 5: float32 [2048, 256], replicated
- output 6: float32 [8, 256, 2048], replicated
All inputs are finite; a program needn't handle non-finite values.
Results may differ from the reference program's by a relative error of at most 0.0193.
Values are sent between devices in bfloat16 or wider.
A program may use at most 1 GiB of HBM per device.

```python
import jax
import jax.numpy as jnp
from jax import lax

BATCH_SIZE = 16
SEQ_LEN = 1024
MODEL_DIM = 2048
NUM_HEADS = 8
HEAD_DIM = 256

HALF_DIM = HEAD_DIM // 2
SCORE_SCALE = HEAD_DIM ** -0.5


def setup_inputs(seed: int = 0) -> dict:
    keys = jax.random.split(jax.random.key(seed), 6)
    act_shape = (BATCH_SIZE, SEQ_LEN, MODEL_DIM)
    hidden = jax.random.normal(keys[0], act_shape, jnp.float32)
    d_out = jax.random.normal(keys[1], act_shape, jnp.float32)
    w_query = jax.random.normal(keys[2], (MODEL_DIM, NUM_HEADS, HEAD_DIM), jnp.float32) * MODEL_DIM ** -0.5
    w_key = jax.random.normal(keys[3], (MODEL_DIM, HEAD_DIM), jnp.float32) * MODEL_DIM ** -0.5
    w_value = jax.random.normal(keys[4], (MODEL_DIM, HEAD_DIM), jnp.float32) * MODEL_DIM ** -0.5
    w_out = jax.random.normal(keys[5], (NUM_HEADS, HEAD_DIM, MODEL_DIM), jnp.float32) * (NUM_HEADS * HEAD_DIM) ** -0.5
    return {'hidden': hidden.astype(jnp.bfloat16), 'd_out': d_out.astype(jnp.bfloat16), 'w_query': w_query.astype(jnp.bfloat16), 'w_key': w_key.astype(jnp.bfloat16), 'w_value': w_value.astype(jnp.bfloat16), 'w_out': w_out.astype(jnp.bfloat16)}


def rope_tables(positions):
    inv_freq = 10000.0 ** (-(jnp.arange(HALF_DIM).astype(jnp.float32) * 2.0) / HEAD_DIM)
    angles = positions.astype(jnp.float32)[:, None] * inv_freq[None, :]
    return jnp.cos(angles), jnp.sin(angles)


def rotate(values, cos_tab, sin_tab):
    lead_half, tail_half = values[..., :HALF_DIM], values[..., HALF_DIM:]
    return jnp.concatenate([lead_half * cos_tab - tail_half * sin_tab, tail_half * cos_tab + lead_half * sin_tab], axis=-1)


def rotate_back(cotangent, cos_tab, sin_tab):
    lead_half, tail_half = cotangent[..., :HALF_DIM], cotangent[..., HALF_DIM:]
    return jnp.concatenate([lead_half * cos_tab + tail_half * sin_tab, tail_half * cos_tab - lead_half * sin_tab], axis=-1)


def causal_softmax(scores):
    row_max = jnp.max(scores, axis=-1, keepdims=True)
    expo_vals = jnp.exp(scores - row_max)
    return expo_vals / jnp.sum(expo_vals, axis=-1, keepdims=True)


def reference(hidden, d_out, w_query, w_key, w_value, w_out):
    cos_tab, sin_tab = rope_tables(jnp.arange(SEQ_LEN))
    hidden_wide = hidden.astype(jnp.float32)
    q_proj = jnp.einsum('bld,dhe->blhe', hidden_wide, w_query.astype(jnp.float32)).astype(jnp.bfloat16)
    k_proj = jnp.einsum('bld,de->ble', hidden_wide, w_key.astype(jnp.float32)).astype(jnp.bfloat16)
    v_proj = jnp.einsum('bld,de->ble', hidden_wide, w_value.astype(jnp.float32)).astype(jnp.bfloat16)
    q_rot = rotate(q_proj.astype(jnp.float32), cos_tab[:, None, :], sin_tab[:, None, :]).astype(jnp.bfloat16)
    k_rot = rotate(k_proj.astype(jnp.float32), cos_tab, sin_tab).astype(jnp.bfloat16)
    k_wide = k_rot.astype(jnp.float32)
    v_wide = v_proj.astype(jnp.float32)
    causal = jnp.arange(SEQ_LEN)[:, None] >= jnp.arange(SEQ_LEN)[None, :]

    def head_probs(q_head):
        scores = jnp.einsum('bqe,bke->bqk', q_head.astype(jnp.float32), k_wide) * SCORE_SCALE
        return causal_softmax(jnp.where(causal, scores, -jnp.inf))

    def head_forward(q_head):
        attn_prob = head_probs(q_head)
        return jnp.einsum('bqk,bke->bqe', attn_prob.astype(jnp.bfloat16).astype(jnp.float32), v_wide).astype(jnp.bfloat16)

    q_heads = jnp.moveaxis(q_rot, 2, 0)
    attn = lax.map(head_forward, q_heads)
    attn_wide = attn.astype(jnp.float32)
    w_out_wide = w_out.astype(jnp.float32)
    attn_out = jnp.einsum('hble,hed->bld', attn_wide, w_out_wide).astype(jnp.bfloat16)
    d_out_wide = d_out.astype(jnp.float32)
    d_attn = jnp.einsum('bld,hed->hble', d_out_wide, w_out_wide).astype(jnp.bfloat16)

    def head_backward(acc_pair, head_slices):
        q_head, attn_head, d_head = head_slices
        attn_prob = head_probs(q_head)
        d_head_wide = d_head.astype(jnp.float32)
        d_prob = jnp.einsum('bqe,bke->bqk', d_head_wide, v_wide)
        row_delta = jnp.sum(d_head_wide * attn_head.astype(jnp.float32), axis=-1, keepdims=True)
        d_scores = (attn_prob * (d_prob - row_delta) * SCORE_SCALE).astype(jnp.bfloat16).astype(jnp.float32)
        dq_head = jnp.einsum('bqk,bke->bqe', d_scores, k_wide).astype(jnp.bfloat16)
        dk_acc = acc_pair[0] + jnp.einsum('bqk,bqe->bke', d_scores, q_head.astype(jnp.float32))
        dv_acc = acc_pair[1] + jnp.einsum('bqk,bqe->bke', attn_prob.astype(jnp.bfloat16).astype(jnp.float32), d_head_wide)
        return (dk_acc, dv_acc), dq_head

    zero_acc = jnp.zeros((BATCH_SIZE, SEQ_LEN, HEAD_DIM), jnp.float32)
    (dk_sum, dv_sum), dq_heads = lax.scan(head_backward, (zero_acc, zero_acc), (q_heads, attn, d_attn))
    d_query = rotate_back(jnp.moveaxis(dq_heads, 0, 2).astype(jnp.float32), cos_tab[:, None, :], sin_tab[:, None, :]).astype(jnp.bfloat16)
    d_key = rotate_back(dk_sum.astype(jnp.bfloat16).astype(jnp.float32), cos_tab, sin_tab).astype(jnp.bfloat16)
    d_value = dv_sum.astype(jnp.bfloat16)
    dq_wide = d_query.astype(jnp.float32)
    dk_wide = d_key.astype(jnp.float32)
    dv_wide = d_value.astype(jnp.float32)
    d_hidden = (jnp.einsum('blhe,dhe->bld', dq_wide, w_query.astype(jnp.float32)) + jnp.einsum('ble,de->bld', dk_wide, w_key.astype(jnp.float32)) + jnp.einsum('ble,de->bld', dv_wide, w_value.astype(jnp.float32))).astype(jnp.bfloat16)
    grad_w_query = jnp.einsum('bld,blhe->dhe', hidden_wide, dq_wide)
    grad_w_key = jnp.einsum('bld,ble->de', hidden_wide, dk_wide)
    grad_w_value = jnp.einsum('bld,ble->de', hidden_wide, dv_wide)
    grad_w_out = jnp.einsum('hble,bld->hed', attn_wide, d_out_wide)
    return (attn_out, d_hidden, grad_w_query, grad_w_key, grad_w_value, grad_w_out)
```

```python
import functools

import jax
import jax.numpy as jnp
from jax import lax
from jax.experimental import pallas as pl
from jax.experimental.pallas import tpu as pltpu
from jax.sharding import PartitionSpec as P

F32 = jnp.float32
BF16 = jnp.bfloat16
NT = (((1,), (1,)), ((), ()))
NN = (((1,), (0,)), ((), ()))
TN = (((0,), (0,)), ((), ()))
LOG2E = 1.4426950408889634
CHIP_BLOCKS = ((0,), (0, 1), (0, 2, 3), (0, 1, 2, 3))


def dot(a, b, dims):
    return lax.dot_general(a, b, dims, preferred_element_type=F32)


def rope_tables(positions, head_dim):
    half_dim = head_dim // 2
    inv_freq = 10000.0 ** (-(jnp.arange(half_dim).astype(F32) * 2.0) / head_dim)
    angles = positions.astype(F32)[:, None] * inv_freq[None, :]
    return jnp.cos(angles), jnp.sin(angles)


def rotate(x, cos, sin, sign):
    half = x.shape[-1] // 2
    a, b = x[..., :half].astype(F32), x[..., half:].astype(F32)
    s = sin * sign
    return jnp.concatenate([a * cos - b * s, b * cos + a * s], axis=-1).astype(BF16)


def attn_step(blocks, heads, hd, scale, core, first, q_refs, do_refs, kv_refs, k_rot, cos_ref, sin_ref, o_refs, dq_refs, dkv_refs):
    half_rows = q_refs[0].shape[1]
    rows = 2 * half_rows
    flip = core * half_rows
    pos = lambda t: jnp.where(t < half_rows, t + flip, t - flip)
    cos, sin = cos_ref[:rows], sin_ref[:rows]

    @pl.when(first)
    def _():
        for b in blocks:
            tab = slice(b * rows, (b + 1) * rows)
            k_rot[b] = rotate(kv_refs[b][0, :, :hd], cos_ref[tab], sin_ref[tab], 1.0)

    keep = pos(lax.broadcasted_iota(jnp.int32, (rows, rows), 0)) >= pos(lax.broadcasted_iota(jnp.int32, (rows, rows), 1))
    for h in range(heads):
        cols = slice(h * hd, (h + 1) * hd)
        q = rotate(jnp.concatenate([q_refs[0][0, :, cols], q_refs[1][0, :, cols]], axis=0), cos, sin, 1.0)
        do = jnp.concatenate([do_refs[0][0, :, cols], do_refs[1][0, :, cols]], axis=0)
        s = [dot(q, k_rot[b], NT) for b in blocks]
        s[0] = jnp.where(keep, s[0], -jnp.inf)
        m = functools.reduce(jnp.maximum, [jnp.max(t, axis=1, keepdims=True) for t in s])
        e = [jnp.exp2((t - m) * (scale * LOG2E)) for t in s]
        inv = 1.0 / functools.reduce(jnp.add, [jnp.sum(t, axis=1, keepdims=True) for t in e])
        p = [t * inv for t in e]
        pb = [t.astype(BF16) for t in p]
        o = functools.reduce(jnp.add, [dot(pb[i], kv_refs[b][0, :, hd:], NN) for i, b in enumerate(blocks)]).astype(BF16)
        o_refs[0][0, :, cols] = o[:half_rows]
        o_refs[1][0, :, cols] = o[half_rows:]
        delta = jnp.sum(do.astype(F32) * o.astype(F32), axis=1, keepdims=True)
        ds = [(p[i] * (dot(do, kv_refs[b][0, :, hd:], NT) - delta) * scale).astype(BF16) for i, b in enumerate(blocks)]
        dq = functools.reduce(jnp.add, [dot(ds[i], k_rot[b], NN) for i, b in enumerate(blocks)]).astype(BF16)
        dq = rotate(dq, cos, sin, -1.0)
        dq_refs[0][0, :, cols] = dq[:half_rows]
        dq_refs[1][0, :, cols] = dq[half_rows:]
        for i, b in enumerate(blocks):
            dk = dot(ds[i], q, TN)
            dv = dot(pb[i], do, TN)
            if h == 0:
                @pl.when(first)
                def _():
                    dkv_refs[b][0, :, :hd] = dk
                    dkv_refs[b][0, :, hd:] = dv

                @pl.when(jnp.logical_not(first))
                def _():
                    dkv_refs[b][0, :, :hd] += dk
                    dkv_refs[b][0, :, hd:] += dv
            else:
                dkv_refs[b][0, :, :hd] += dk
                dkv_refs[b][0, :, hd:] += dv


def attn_kernel(heads, hd, chained, ids, q0, q1, d0, d1, kv0, kv1, kv2, kv3, cos, sin, *rest):
    o0, o1, g0, g1, w0, w1, w2, w3, k_rot = rest[2 * chained:]
    kv_refs = (kv0, kv1, kv2, kv3)
    dkv_refs = (w0, w1, w2, w3)
    chip, core = ids[0], ids[1]
    first = pl.program_id(1) == 0
    for c, blocks in enumerate(CHIP_BLOCKS):
        @pl.when(chip == c)
        def _():
            attn_step(blocks, heads, hd, hd ** -0.5, core, first, (q0, q1), (d0, d1), kv_refs, k_rot, cos, sin, (o0, o1), (g0, g1), dkv_refs)
            for b in range(4):
                if b not in blocks:
                    @pl.when(first)
                    def _():
                        dkv_refs[b][...] = jnp.zeros_like(dkv_refs[b])


def attention(ids, start, q, q_in, do, do_in, kvs, cos, sin, hd, full=None, heads=2):
    cs, rows = kvs[0].shape[:2]
    total, half_rows, width = q_in.shape
    mine = pl.BlockSpec((1, half_rows, heads * hd), lambda b, h, ids: (ids[1] * total + start + b, 0, h))
    other = pl.BlockSpec((1, half_rows, heads * hd), lambda b, h, ids: (start + b, 0, h))
    part = pl.BlockSpec((1, half_rows, heads * hd), lambda b, h, ids: (b, 0, h))
    kv_spec = pl.BlockSpec((1, rows, 2 * hd), lambda b, h, ids: (b, 0, 0))
    tab = pl.BlockSpec((4 * rows, hd // 2), lambda b, h, ids: (0, 0))
    whole = jax.ShapeDtypeStruct((2 * total, half_rows, width), BF16)
    act = jax.ShapeDtypeStruct((cs, half_rows, width), BF16)
    acc = jax.ShapeDtypeStruct((cs, rows, 2 * hd), F32)
    chained = full is not None
    extra = list(full) if chained else []
    return pl.pallas_call(
        functools.partial(attn_kernel, heads, hd, chained),
        grid_spec=pltpu.PrefetchScalarGridSpec(
            num_scalar_prefetch=1,
            grid=(cs, width // (heads * hd)),
            in_specs=[mine, other, mine, other, kv_spec, kv_spec, kv_spec, kv_spec, tab, tab] + [pl.BlockSpec(memory_space=pl.ANY)] * len(extra),
            out_specs=[mine, part, mine, part] + [kv_spec] * 4,
            scratch_shapes=[pltpu.VMEM((4, rows, hd), BF16)],
        ),
        out_shape=[whole, act, whole, act] + [acc] * 4,
        input_output_aliases={11: 0, 12: 2} if chained else {},
        compiler_params=pltpu.CompilerParams(dimension_semantics=("arbitrary", "arbitrary"), vmem_limit_bytes=56 * 1024 * 1024),
        cost_estimate=pl.CostEstimate(flops=6 * 2 * cs * rows * width * rows * 8, bytes_accessed=30 * 1024 * 1024, transcendentals=0),
        name="attention",
    )(ids, q, q_in, do, do_in, *kvs, cos, sin, *extra)


MESH = pl.DeviceIdType.MESH
PIECE = 512


def remote(src, dst, sems, i, dev):
    return pltpu.make_async_remote_copy(src_ref=src, dst_ref=dst, send_sem=sems.at[0, i], recv_sem=sems.at[1, i], device_id=(dev,), device_id_type=MESH)


def sum_kernel(counts, *refs):
    ng = len(counts)
    g_refs, out_refs = refs[:ng], refs[ng:2 * ng]
    h, dr, r1, r2, load_sem, keep_sem, d_sem, s1_sem, s2_sem, g1_sem, g2_sem, g3_sem = refs[2 * ng:]
    dev = lax.axis_index('sp')
    chip, core = dev // 2, dev % 2
    bits = (chip % 2, chip // 2)
    partner = dev + 1 - 2 * core
    across = (dev + 2 - 4 * bits[0], dev + 4 - 8 * bits[1])
    half, quarter, eighth, last = PIECE // 2, PIECE // 4, PIECE // 8, PIECE // 16

    barrier = pltpu.get_barrier_semaphore()
    for d in (partner,) + across:
        pl.semaphore_signal(barrier, inc=1, device_id=(d,), device_id_type=MESH)
    pl.semaphore_wait(barrier, 3)

    def rows(ref, start, size):
        return ref.at[pl.ds(pl.multiple_of(start, 32), size)]

    def each(body):
        base = 0
        for i, count in enumerate(counts):
            def step(p, carry, i=i, base=base):
                body(i, p, base + p)
                return carry
            lax.fori_loop(0, count, step, 0)
            base += count

    def load(i, p, s):
        return pltpu.make_async_copy(rows(g_refs[i], p * PIECE + core * half, half), h.at[s], load_sem.at[s])

    def cross(i, p, s):
        return remote(rows(g_refs[i], p * PIECE + (1 - core) * half, half), dr.at[s], d_sem, s, partner)

    def first(w, s):
        src = h.at[s, pl.ds(pl.multiple_of(w * quarter + (1 - bits[w]) * eighth, 32), eighth)]
        return remote(src, r1.at[w, s], s1_sem.at[w], s, across[w])

    def second(w, s):
        src = h.at[s, pl.ds(pl.multiple_of(w * quarter + bits[w] * eighth + (1 - bits[1 - w]) * last, 32), last)]
        return remote(src, r2.at[w, s], s2_sem.at[w], s, across[1 - w])

    def kept(w):
        return w * quarter + bits[w] * eighth

    def final(w):
        return kept(w) + bits[1 - w] * last

    def keep(w, i, p, s):
        return pltpu.make_async_copy(h.at[s, pl.ds(pl.multiple_of(final(w), 32), last)], rows(out_refs[i], p * PIECE + core * half + final(w), last), keep_sem.at[w, s])

    def share1(w, i, p, s):
        return remote(h.at[s, pl.ds(pl.multiple_of(final(w), 32), last)], rows(out_refs[i], p * PIECE + core * half + final(w), last), g1_sem.at[w], s, across[1 - w])

    def share2(w, i, p, s):
        here = rows(out_refs[i], p * PIECE + core * half + kept(w), eighth)
        return remote(here, here, g2_sem.at[w], s, across[w])

    def share3(i, p, s):
        here = rows(out_refs[i], p * PIECE + core * half, half)
        return remote(here, here, g3_sem, s, partner)

    def begin(i, p, s):
        cross(i, p, s).start()
        load(i, p, s).start()

    def phase1(i, p, s):
        load(i, p, s).wait()
        cross(i, p, s).wait()

        @pl.loop(0, half, step=32)
        def _(r):
            at = pl.ds(pl.multiple_of(r, 32), 32)
            h[s, at] += dr[s, at]
        for w in range(2):
            first(w, s).start()

    def phase2(i, p, s):
        for w in range(2):
            first(w, s).wait()
            at = pl.ds(pl.multiple_of(kept(w), 32), eighth)
            h[s, at] += r1[w, s]
            second(w, s).start()

    def phase3(i, p, s):
        for w in range(2):
            second(w, s).wait()
            at = pl.ds(pl.multiple_of(final(w), 32), last)
            h[s, at] += r2[w, s]
            share1(w, i, p, s).start()
            keep(w, i, p, s).start()

    def phase4(i, p, s):
        for w in range(2):
            share1(w, i, p, s).wait()
            keep(w, i, p, s).wait()
            share2(w, i, p, s).start()

    def phase5(i, p, s):
        for w in range(2):
            share2(w, i, p, s).wait()
        share3(i, p, s).start()

    def phase6(i, p, s):
        share3(i, p, s).wait()

    for phase in (begin, phase1, phase2, phase3, phase4, phase5, phase6):
        each(phase)


def sum_all(grads):
    counts = tuple(g.shape[0] // PIECE for g in grads)
    total = sum(counts)
    width = grads[0].shape[1]
    dma = pltpu.SemaphoreType.DMA
    return pl.pallas_call(
        functools.partial(sum_kernel, counts),
        out_shape=[jax.ShapeDtypeStruct(g.shape, F32) for g in grads],
        in_specs=[pl.BlockSpec(memory_space=pl.ANY)] * len(grads),
        out_specs=[pl.BlockSpec(memory_space=pl.ANY)] * len(grads),
        scratch_shapes=[
            pltpu.VMEM((total, PIECE // 2, width), F32),
            pltpu.VMEM((total, PIECE // 2, width), F32),
            pltpu.VMEM((2, total, PIECE // 8, width), F32),
            pltpu.VMEM((2, total, PIECE // 16, width), F32),
            dma((total,)), dma((2, total)), dma((2, total)),
            dma((2, 2, total)), dma((2, 2, total)), dma((2, 2, total)), dma((2, 2, total)), dma((2, total)),
        ],
        compiler_params=pltpu.CompilerParams(collective_id=1, has_side_effects=True, vmem_limit_bytes=60 * 1024 * 1024),
        name="sum_all",
    )(*grads)


CHUNKS = 4
BARRIER = False


def solution(mesh):
    n = mesh.shape['sp']
    seq_spec = P(None, 'sp', None)
    rep_spec = P()

    def shift(x, bit, chips=None):
        return lax.ppermute(x, 'sp', [(d, d ^ bit) for d in range(n) if chips is None or d // 2 in chips])

    def local_step(hidden, d_out, w_query, w_key, w_value, w_out):
        batch, local_len, width = hidden.shape
        hd = w_key.shape[1]
        qw = w_query.shape[1] * hd
        nb = batch // 2
        dev = lax.axis_index('sp')
        chip, core = dev // 2, dev % 2
        ids = jnp.stack([chip, core]).astype(jnp.int32)
        wq = w_query.reshape(width, qw)
        wo = w_out.reshape(qw, width)
        wkv = jnp.concatenate([w_key, w_value], axis=1)
        mine, yours = core * nb, (1 - core) * nb
        take = lambda x, i: lax.dynamic_slice_in_dim(x, i, nb, 0)
        put = lambda x, y, i: lax.dynamic_update_slice_in_dim(x, y, i, 0)

        offset = jnp.arange(local_len)
        positions = [((dev ^ (2 * b)) ^ c) * local_len + offset for b in range(4) for c in range(2)]
        cos, sin = rope_tables(jnp.concatenate(positions), hd)
        rows = 2 * local_len

        proj = lambda x, w, eq: jnp.einsum(eq, x, w, preferred_element_type=F32).astype(BF16)
        kv = proj(hidden, wkv, 'bld,de->ble')
        kv_own = jnp.concatenate([take(kv, mine), shift(take(kv, yours), 1)], axis=1)
        cs = nb // CHUNKS
        hb = cs // 2
        kvs = []
        for j in range(CHUNKS):
            own = kv_own[j * cs:(j + 1) * cs]
            kx, ky = shift(own, 2), shift(own, 4)
            kvs.append((own, kx, ky, jnp.concatenate([shift(ky[:hb], 2), shift(kx[hb:], 4)], axis=0)))

        do = proj(d_out, wo, 'bld,ed->ble')
        do_in = shift(take(do, yours), 1)
        q = proj(hidden, wq, 'bld,de->ble')
        q_in = shift(take(q, yours), 1)

        full = None
        backs, dkvs = [], []
        for j in range(CHUNKS):
            if j > 1:
                full = tuple(put(f, b, yours + (j - 2) * cs) for f, b in zip(full, backs[j - 2]))
            o, o_oth, dq, dq_oth, w_own, w_x, w_y, w_d = attention(ids, j * cs, q, q_in, do, do_in, kvs[j], cos, sin, hd, full)
            full = (o, dq)
            backs.append((shift(o_oth, 1), shift(dq_oth, 1)))
            r_a = shift(w_d[:hb], 2, (2, 3))
            r_b = shift(w_d[hb:], 4, (2, 3))
            y_b = shift(w_y[hb:], 4, (2, 3))
            x_a = shift(w_x[:hb], 2, (1, 3))
            y_a = shift(w_y[:hb] + r_a, 4, (2, 3))
            x_b = shift(w_x[hb:] + r_b, 2, (0, 1, 3))
            dkvs.append((w_own + jnp.concatenate([y_a + x_a, y_b + x_b], axis=0)).astype(BF16))
        for j in range(max(CHUNKS - 2, 0), CHUNKS):
            full = tuple(put(f, b, yours + j * cs) for f, b in zip(full, backs[j]))
        o, dq = full

        grad = lambda x, y: jnp.einsum('bld,ble->de', x, y, preferred_element_type=F32)
        grad_wo, grad_wq = grad(o, d_out), grad(hidden, dq)
        attn_out = proj(o, wo, 'ble,ed->bld')

        dkv = jnp.concatenate(dkvs, axis=0)
        dkv = jnp.concatenate([rotate(dkv[..., :hd], cos[:rows], sin[:rows], -1.0), dkv[..., hd:]], axis=-1)
        dkv_back = shift(dkv[:, local_len:], 1)
        dkv = dkv[:, :local_len]
        first, second = jnp.where(core == 0, dkv, dkv_back), jnp.where(core == 0, dkv_back, dkv)
        dkv = jnp.concatenate([first, second], axis=0)
        grad_wkv = grad(dkv, hidden)
        part = jnp.einsum('ble,de->bld', dq, wq, preferred_element_type=F32)
        d_hidden = (part + jnp.einsum('ble,de->bld', dkv, wkv, preferred_element_type=F32)).astype(BF16)
        if BARRIER:
            grad_wo, grad_wq, grad_wkv, attn_out, d_hidden = lax.optimization_barrier((grad_wo, grad_wq, grad_wkv, attn_out, d_hidden))
        grad_wo, grad_wq, grad_wkv = sum_all((grad_wo, grad_wq, grad_wkv))
        return (attn_out, d_hidden, grad_wq.reshape(w_query.shape), grad_wkv[:hd].T, grad_wkv[hd:].T, grad_wo.reshape(w_out.shape))

    return jax.shard_map(local_step, mesh=mesh, in_specs=(seq_spec, seq_spec, rep_spec, rep_spec, rep_spec, rep_spec), out_specs=(seq_spec, seq_spec, rep_spec, rep_spec, rep_spec, rep_spec), check_vma=False)
```

```python
import functools

import jax
import jax.numpy as jnp
from jax import lax
from jax.experimental import pallas as pl
from jax.experimental.pallas import tpu as pltpu
from jax.sharding import PartitionSpec as P

F32 = jnp.float32
BF16 = jnp.bfloat16
NT = (((1,), (1,)), ((), ()))
NN = (((1,), (0,)), ((), ()))
TN = (((0,), (0,)), ((), ()))
LOG2E = 1.4426950408889634
CHIP_BLOCKS = ((0,), (0, 1), (0, 2, 3), (0, 1, 2, 3))


def dot(a, b, dims):
    return lax.dot_general(a, b, dims, preferred_element_type=F32)


def rope_tables(positions, head_dim):
    half_dim = head_dim // 2
    inv_freq = 10000.0 ** (-(jnp.arange(half_dim).astype(F32) * 2.0) / head_dim)
    angles = positions.astype(F32)[:, None] * inv_freq[None, :]
    return jnp.cos(angles), jnp.sin(angles)


def rotate(x, cos, sin, sign):
    half = x.shape[-1] // 2
    a, b = x[..., :half].astype(F32), x[..., half:].astype(F32)
    s = sin * sign
    return jnp.concatenate([a * cos - b * s, b * cos + a * s], axis=-1).astype(BF16)


def attn_step(blocks, heads, hd, scale, core, first, s, step, q_refs, do_refs, kv, k_rot, cos_ref, sin_ref, stage, slot, acc):
    rows = kv.shape[2]
    half_rows = rows // 2
    flip = core * half_rows
    pos = lambda t: jnp.where(t < half_rows, t + flip, t - flip)
    cos, sin = cos_ref[:rows], sin_ref[:rows]

    @pl.when(first)
    def _():
        for b in blocks:
            tab = slice(b * rows, (b + 1) * rows)
            k_rot[b] = rotate(kv[b, s, :, :hd], cos_ref[tab], sin_ref[tab], 1.0)

    keep = pos(lax.broadcasted_iota(jnp.int32, (rows, rows), 0)) >= pos(lax.broadcasted_iota(jnp.int32, (rows, rows), 1))
    for h in range(heads):
        cols = slice(h * hd, (h + 1) * hd)
        wide = pl.ds(pl.multiple_of((step * heads + h) * hd, hd), hd)
        q = rotate(jnp.concatenate([q_refs[0][0, :, cols], q_refs[1][s, :, wide]], axis=0), cos, sin, 1.0)
        do = jnp.concatenate([do_refs[0][0, :, cols], do_refs[1][s, :, wide]], axis=0)
        sc = [dot(q, k_rot[b], NT) for b in blocks]
        sc[0] = jnp.where(keep, sc[0], -jnp.inf)
        m = functools.reduce(jnp.maximum, [jnp.max(t, axis=1, keepdims=True) for t in sc])
        e = [jnp.exp2((t - m) * (scale * LOG2E)) for t in sc]
        inv = 1.0 / functools.reduce(jnp.add, [jnp.sum(t, axis=1, keepdims=True) for t in e])
        p = [t * inv for t in e]
        pb = [t.astype(BF16) for t in p]
        o = functools.reduce(jnp.add, [dot(pb[i], kv[b, s, :, hd:], NN) for i, b in enumerate(blocks)]).astype(BF16)
        stage[slot, 0, 0, :, wide] = o[:half_rows]
        stage[slot, 0, 1, :, wide] = o[half_rows:]
        delta = jnp.sum(do.astype(F32) * o.astype(F32), axis=1, keepdims=True)
        ds = [(p[i] * (dot(do, kv[b, s, :, hd:], NT) - delta) * scale).astype(BF16) for i, b in enumerate(blocks)]
        dq = functools.reduce(jnp.add, [dot(ds[i], k_rot[b], NN) for i, b in enumerate(blocks)]).astype(BF16)
        dq = rotate(dq, cos, sin, -1.0)
        stage[slot, 1, 0, :, wide] = dq[:half_rows]
        stage[slot, 1, 1, :, wide] = dq[half_rows:]
        for i, b in enumerate(blocks):
            dk = dot(ds[i], q, TN)
            dv = dot(pb[i], do, TN)
            if h == 0:
                @pl.when(first)
                def _():
                    acc[b, s, :, :hd] = dk
                    acc[b, s, :, hd:] = dv

                @pl.when(jnp.logical_not(first))
                def _():
                    acc[b, s, :, :hd] += dk
                    acc[b, s, :, hd:] += dv
            else:
                acc[b, s, :, :hd] += dk
                acc[b, s, :, hd:] += dv


MESH = pl.DeviceIdType.MESH
PIECE = 512


def remote(src, dst, sems, i, dev):
    return pltpu.make_async_remote_copy(src_ref=src, dst_ref=dst, send_sem=sems.at[0, i], recv_sem=sems.at[1, i], device_id=(dev,), device_id_type=MESH)


def sum_kernel(counts, *refs):
    ng = len(counts)
    hid_ref, dout_ref, o_ref, wo_ref, dq_ref, wq_ref, dkv_ref, wkv_ref = refs[:8]
    out_refs, (attn_out, d_hidden, dr) = refs[8:ng + 8], refs[ng + 8:ng + 11]
    h, dv, give, flip, r1, r2, xs, ws, xs2, ws2, tiles, dr_sem, mm_sem, tile_sem, keep_sem, d_sem, s1_sem, s2_sem, g1_sem, g2_sem, g3_sem = refs[ng + 11:]
    total = sum(counts)
    dev = lax.axis_index('sp')
    chip, core = dev // 2, dev % 2
    bits = (chip % 2, chip // 2)
    partner = dev + 1 - 2 * core
    across = (dev + 2 - 4 * bits[0], dev + 4 - 8 * bits[1])
    half, quarter, eighth, last = PIECE // 2, PIECE // 4, PIECE // 8, PIECE // 16

    barrier = pltpu.get_barrier_semaphore()
    for d in (partner,) + across:
        pl.semaphore_signal(barrier, inc=1, device_id=(d,), device_id_type=MESH)
    pl.semaphore_wait(barrier, 3)

    def rows(ref, start, size):
        return ref.at[pl.ds(pl.multiple_of(start, 32), size)]

    def each(body, which=range(ng)):
        base = 0
        for i, count in enumerate(counts):
            def step(p, carry, i=i, base=base):
                body(i, p, base + p)
                return carry
            if i in which:
                lax.fori_loop(0, count, step, 0)
            base += count

    def cross(s):
        return remote(give.at[s % 2], dr.at[s], d_sem, s, partner)

    def first(w, s):
        src = h.at[s, pl.ds(pl.multiple_of(w * quarter + (1 - bits[w]) * eighth, 32), eighth)]
        return remote(src, r1.at[w, s], s1_sem.at[w], s, across[w])

    def second(w, s):
        src = h.at[s, pl.ds(pl.multiple_of(w * quarter + bits[w] * eighth + (1 - bits[1 - w]) * last, 32), last)]
        return remote(src, r2.at[w, s], s2_sem.at[w], s, across[1 - w])

    def kept(w):
        return w * quarter + bits[w] * eighth

    def final(w):
        return kept(w) + bits[1 - w] * last

    def keep(w, i, p, s):
        return pltpu.make_async_copy(h.at[s, pl.ds(pl.multiple_of(final(w), 32), last)], rows(out_refs[i], p * PIECE + core * half + final(w), last), keep_sem.at[w, s])

    def share1(w, i, p, s):
        return remote(h.at[s, pl.ds(pl.multiple_of(final(w), 32), last)], rows(out_refs[i], p * PIECE + core * half + final(w), last), g1_sem.at[w], s, across[1 - w])

    def share2(w, i, p, s):
        here = rows(out_refs[i], p * PIECE + core * half + kept(w), eighth)
        return remote(here, here, g2_sem.at[w], s, across[w])

    def share3(i, p, s):
        here = rows(out_refs[i], p * PIECE + core * half, half)
        return remote(here, here, g3_sem, s, partner)

    def product_rows(left, right, start, put):
        cols = pl.ds(pl.multiple_of(start, half), half)

        @pl.loop(0, left.shape[0], step=half)
        def _(r):
            at = pl.ds(pl.multiple_of(r, half), half)
            flip[:, at] = left[at, cols].T

        @pl.loop(0, right.shape[1], step=512)
        def _(c):
            at = pl.ds(pl.multiple_of(c, 512), 512)
            put(at, dot(flip[...], right[:, at], NN))

    def phase1(left, right, i, p, s):
        @pl.when(s >= 2)
        def _():
            cross(s - 2).wait_send()

        def put_give(at, x):
            give[s % 2, :, at] = x

        def put_keep(at, x):
            h[s, :, at] = x
        product_rows(left, right, p * PIECE + (1 - core) * half, put_give)
        cross(s).start()
        product_rows(left, right, p * PIECE + core * half, put_keep)
        cross(s).wait_recv()
        fetch = pltpu.make_async_copy(dr.at[s], dv, dr_sem)
        fetch.start()
        fetch.wait()

        @pl.loop(0, half, step=32)
        def _(r):
            at = pl.ds(pl.multiple_of(r, 32), 32)
            h[s, at] += dv[at]
        for w in range(2):
            first(w, s).start()

    def phase2(i, p, s):
        for w in range(2):
            first(w, s).wait()
            at = pl.ds(pl.multiple_of(kept(w), 32), eighth)
            h[s, at] += r1[w, s]
            second(w, s).start()

    def phase3(i, p, s):
        for w in range(2):
            second(w, s).wait()
            at = pl.ds(pl.multiple_of(final(w), 32), last)
            h[s, at] += r2[w, s]
            share1(w, i, p, s).start()
            keep(w, i, p, s).start()

    def phase4(i, p, s):
        for w in range(2):
            share1(w, i, p, s).wait()
            keep(w, i, p, s).wait()
            share2(w, i, p, s).start()

    def phase5(i, p, s):
        for w in range(2):
            share2(w, i, p, s).wait()
        share3(i, p, s).start()

    def phase6(i, p, s):
        share3(i, p, s).wait()

    tm, tn = tiles.shape[1:]
    across_n = ws.shape[0] // tn
    n_tiles = xs.shape[0] // tm * across_n

    def bring(src, dst, k):
        return pltpu.make_async_copy(src, dst, mm_sem.at[k])

    def spill(out, t):
        at = (pl.ds(pl.multiple_of(t // across_n * tm, tm), tm), pl.ds(pl.multiple_of(t % across_n * tn, tn), tn))
        return pltpu.make_async_copy(tiles.at[t % 2], out.at[at], tile_sem.at[t % 2])

    def matmul(out, product):
        @pl.loop(0, n_tiles)
        def _(t):
            @pl.when(t >= 2)
            def _():
                spill(out, t - 2).wait()
            m, c = pl.ds(pl.multiple_of(t // across_n * tm, tm), tm), pl.ds(pl.multiple_of(t % across_n * tn, tn), tn)
            tiles[t % 2] = product(m, c).astype(BF16)
            spill(out, t).start()
        for t in (n_tiles - 2, n_tiles - 1):
            spill(out, t).wait()

    def forward(m, c):
        return dot(ws[m], xs[:, c], NN)

    def backward(m, c):
        return dot(ws[m], xs[c], NT) + dot(xs2[m], ws2[c], NT)

    def bring_all(*pairs):
        copies = [bring(src, dst, k) for k, (src, dst) in enumerate(pairs)]
        for copy in copies:
            copy.start()
        for copy in copies:
            copy.wait()

    bring_all((o_ref, xs), (dout_ref, ws))
    each(functools.partial(phase1, xs, ws), (0,))
    bring_all((hid_ref, xs), (dq_ref, ws), (dkv_ref, xs2), (wkv_ref, ws2))
    each(functools.partial(phase1, xs, ws), (1,))
    each(functools.partial(phase1, xs2, xs), (2,))
    for s in (total - 2, total - 1):
        cross(s).wait_send()
    bring_all((wq_ref, xs))
    each(phase2, (0,))
    matmul(d_hidden, backward)
    each(phase2, (1, 2))
    bring_all((o_ref, ws), (wo_ref, xs))
    each(phase3, (0,))
    matmul(attn_out, forward)
    each(phase3, (1, 2))
    for phase in (phase4, phase5, phase6):
        each(phase)


def sum_all(hidden, d_out, o, wo, dq, wq, dkv, wkv):
    grads = [(o.shape[1], d_out.shape[1]), (hidden.shape[1], dq.shape[1]), (dkv.shape[1], hidden.shape[1])]
    counts = tuple(g[0] // PIECE for g in grads)
    total = sum(counts)
    width = grads[0][1]
    dma = pltpu.SemaphoreType.DMA
    hbm = pl.BlockSpec(memory_space=pl.ANY)
    act = jax.ShapeDtypeStruct((o.shape[0], wo.shape[1]), BF16)
    res = pl.pallas_call(
        functools.partial(sum_kernel, counts),
        out_shape=[jax.ShapeDtypeStruct(g, F32) for g in grads] + [act, act, jax.ShapeDtypeStruct((total, PIECE // 2, width), F32)],
        in_specs=[hbm] * 8,
        out_specs=[hbm] * (len(grads) + 3),
        scratch_shapes=[
            pltpu.VMEM((total, PIECE // 2, width), F32),
            pltpu.VMEM((PIECE // 2, width), F32),
            pltpu.VMEM((2, PIECE // 2, width), F32),
            pltpu.VMEM((PIECE // 2, o.shape[0]), BF16),
            pltpu.VMEM((2, total, PIECE // 8, width), F32),
            pltpu.VMEM((2, total, PIECE // 16, width), F32),
            pltpu.VMEM(o.shape, BF16), pltpu.VMEM(wo.shape, BF16),
            pltpu.VMEM(dkv.shape, BF16), pltpu.VMEM(wkv.shape, BF16),
            pltpu.VMEM((2, 512, 256), BF16),
            dma, dma((4,)), dma((2,)), dma((2, total)), dma((2, total)),
            dma((2, 2, total)), dma((2, 2, total)), dma((2, 2, total)), dma((2, 2, total)), dma((2, total)),
        ],
        compiler_params=pltpu.CompilerParams(collective_id=1, has_side_effects=True, vmem_limit_bytes=67 * 1000 * 1000),
        name="sum_all",
    )(hidden, d_out, o, wo, dq, wq, dkv, wkv)
    return res[:-1]


def attn_kernel(heads, hd, lag, q_mine, do_mine, q_all, do_all, kv_all, cos_ref, sin_ref, o_out, dq_out, dkv_out,
                kv, k_rot, q_in, do_in, stage, acc, relay, got, kv_mine_sem, pair_sem, kv_sem, in_sem, keep_sem, give_sem, one_sem, two_sem):
    s, step = pl.program_id(0), pl.program_id(1)
    steps = pl.num_programs(1)
    ns, rows = kv.shape[1], kv.shape[2]
    half_rows = rows // 2
    dev = lax.axis_index('sp')
    chip, core = dev // 2, dev % 2
    bit_x, bit_y = chip % 2, chip // 2
    partner = dev + 1 - 2 * core
    dev_x, dev_y = dev + 2 - 4 * bit_x, dev + 4 - 8 * bit_y
    dev_d = dev_x + 4 - 8 * bit_y
    mine, yours = core * ns, (1 - core) * ns
    slot = s % 2

    def give_kv(b, i):
        return remote(kv.at[0, i], kv.at[b, i], kv_sem.at[b - 1], i, (dev_x, dev_y, dev_d)[b - 1])

    def give_in(i, k):
        return remote((q_all, do_all)[k].at[yours + i], (q_in, do_in)[k].at[i], in_sem.at[k], i, partner)

    up = (bit_x == 0, bit_y == 0, bit_y == 0)
    down = (bit_x == 1, bit_y == 1, bit_y == 1)

    def pair():
        return remote(kv_all.at[pl.ds(yours, ns)], kv.at[0, :, pl.ds(half_rows, half_rows)], pair_sem, 0, partner)

    def own():
        return pltpu.make_async_copy(kv_all.at[pl.ds(mine, ns)], kv.at[0, :, pl.ds(0, half_rows)], kv_mine_sem)

    @pl.when((s == 0) & (step == 0))
    def _():
        barrier = pltpu.get_barrier_semaphore()
        for d in (partner, dev_x, dev_y, dev_d):
            pl.semaphore_signal(barrier, inc=1, device_id=(d,), device_id_type=MESH)
        pl.semaphore_wait(barrier, 4)
        pair().start()
        own().start()
        for k in range(2):
            give_in(0, k).start()
        own().wait()
        pair().wait()

        @pl.loop(0, ns)
        def _(i):
            for b in (1, 2, 3):
                @pl.when(up[b - 1])
                def _():
                    give_kv(b, i).start()

            @pl.when(i > 0)
            def _():
                for k in range(2):
                    give_in(i, k).start()

    def keep(i, k):
        return pltpu.make_async_copy(stage.at[i % 2, k, 0], (o_out, dq_out)[k].at[mine + i], keep_sem.at[k, i % 2])

    def give(i, k):
        return remote(stage.at[i % 2, k, 1], (o_out, dq_out)[k].at[mine + i], give_sem.at[k], i, partner)

    @pl.when(step == 0)
    def _():
        for k in range(2):
            give_in(s, k).wait()
        for b in (1, 2, 3):
            @pl.when(down[b - 1])
            def _():
                give_kv(b, s).wait_recv()

        @pl.when(s >= 2)
        def _():
            for k in range(2):
                keep(s - 2, k).wait()
                give(s - 2, k).wait_send()

    first = step == 0
    for c, blocks in enumerate(CHIP_BLOCKS):
        @pl.when(chip == c)
        def _():
            attn_step(blocks, heads, hd, hd ** -0.5, core, first, s, step, (q_mine, q_in), (do_mine, do_in), kv, k_rot, cos_ref, sin_ref, stage, slot, acc)

    def one(i, w):
        return remote(acc.at[3, i], relay.at[i], one_sem, i, (dev_x, dev_y)[w])

    def two(i, w):
        return remote(acc.at[1 + w, i], got.at[w, i], two_sem.at[w], i, (dev_x, dev_y)[w])

    def send_one(i):
        for w in range(2):
            @pl.when((bit_y == 1) & (i % 2 == w))
            def _():
                one(i, w).start()

    def send_two(i):
        even = i % 2 == 0
        @pl.when(even & (bit_y == 1))
        def _():
            one(i, 0).wait_recv()
            acc[2, i] += relay[i]

        @pl.when(jnp.logical_not(even) & (chip == 1))
        def _():
            one(i, 1).wait_recv()
            acc[1, i] += relay[i]

        @pl.when(jnp.logical_not(even) & (chip == 0))
        def _():
            one(i, 1).wait_recv()
            acc[1, i] = relay[i]

        @pl.when((bit_x == 1) | ((chip == 0) & jnp.logical_not(even)))
        def _():
            two(i, 0).start()

        @pl.when(bit_y == 1)
        def _():
            two(i, 1).start()

    def finish(i):
        even = i % 2 == 0

        @pl.when((bit_x == 0) | ((chip == 1) & jnp.logical_not(even)))
        def _():
            two(i, 0).wait_recv()
            acc[0, i] += got[0, i]

        @pl.when(bit_y == 0)
        def _():
            two(i, 1).wait_recv()
            acc[0, i] += got[1, i]
        total = acc[0, i].astype(BF16)
        dkv_out[i, :, :hd] = rotate(total[:, :hd], cos_ref[:rows], sin_ref[:rows], -1.0)
        dkv_out[i, :, hd:] = total[:, hd:]

    @pl.when(step == steps - 1)
    def _():
        for k in range(2):
            keep(s, k).start()
            give(s, k).start()
        send_one(s)

        @pl.when(s >= lag)
        def _():
            send_two(s - lag)

    @pl.when((s == ns - 1) & (step == steps - 1))
    def _():
        @pl.loop(ns - lag, ns)
        def _(i):
            send_two(i)

        @pl.loop(0, ns)
        def _(i):
            finish(i)
            for k in range(2):
                give(i, k).wait_recv()
            for b in (1, 2, 3):
                @pl.when(up[b - 1])
                def _():
                    give_kv(b, i).wait_send()
            for w in range(2):
                @pl.when((bit_y == 1) & (i % 2 == w))
                def _():
                    one(i, w).wait_send()

            @pl.when((bit_x == 1) | ((chip == 0) & (i % 2 == 1)))
            def _():
                two(i, 0).wait_send()

            @pl.when(bit_y == 1)
            def _():
                two(i, 1).wait_send()
        for i in (ns - 2, ns - 1):
            for k in range(2):
                keep(i, k).wait()
                give(i, k).wait_send()


def attention(q, do, kv, cos, sin, hd, heads=2, lag=1):
    batch, half_rows, width = q.shape
    ns, rows = batch // 2, 2 * half_rows
    mine = pl.BlockSpec((1, half_rows, heads * hd), lambda s, h: (lax.axis_index('sp') % 2 * ns + s, 0, h))
    tab = pl.BlockSpec((4 * rows, hd // 2), lambda s, h: (0, 0))
    hbm = pl.BlockSpec(memory_space=pl.ANY)
    act = jax.ShapeDtypeStruct(q.shape, BF16)
    dma = pltpu.SemaphoreType.DMA
    return pl.pallas_call(
        functools.partial(attn_kernel, heads, hd, lag),
        grid=(ns, width // (heads * hd)),
        in_specs=[mine, mine, hbm, hbm, hbm, tab, tab],
        out_specs=[hbm, hbm, pl.BlockSpec((ns, rows, 2 * hd), lambda s, h: (0, 0, 0))],
        out_shape=[act, act, jax.ShapeDtypeStruct((ns, rows, 2 * hd), BF16)],
        scratch_shapes=[
            pltpu.VMEM((4, ns, rows, 2 * hd), BF16),
            pltpu.VMEM((4, rows, hd), BF16),
            pltpu.VMEM((ns, half_rows, width), BF16),
            pltpu.VMEM((ns, half_rows, width), BF16),
            pltpu.VMEM((2, 2, 2, half_rows, width), BF16),
            pltpu.VMEM((4, ns, rows, 2 * hd), F32),
            pltpu.VMEM((ns, rows, 2 * hd), F32),
            pltpu.VMEM((2, ns, rows, 2 * hd), F32),
            dma, dma((2, 1)), dma((3, 2, ns)), dma((2, 2, ns)), dma((2, 2)), dma((2, 2, ns)), dma((2, ns)), dma((2, 2, ns)),
        ],
        compiler_params=pltpu.CompilerParams(dimension_semantics=("arbitrary", "arbitrary"), collective_id=2, has_side_effects=True, vmem_limit_bytes=66 * 1000 * 1000),
        cost_estimate=pl.CostEstimate(flops=6 * 2 * ns * rows * width * rows * 4, bytes_accessed=100 * 1024 * 1024, transcendentals=0),
        name="attention",
    )(q, do, q, do, kv, cos, sin)


def solution(mesh):
    n = mesh.shape['sp']
    seq_spec = P(None, 'sp', None)
    rep_spec = P()

    def local_step(hidden, d_out, w_query, w_key, w_value, w_out):
        batch, local_len, width = hidden.shape
        hd = w_key.shape[1]
        qw = w_query.shape[1] * hd
        dev = lax.axis_index('sp')
        core = dev % 2
        wq = w_query.reshape(width, qw)
        wo = w_out.reshape(qw, width)
        wkv = jnp.concatenate([w_key, w_value], axis=1)

        offset = jnp.arange(local_len)
        positions = [((dev ^ (2 * b)) ^ c) * local_len + offset for b in range(4) for c in range(2)]
        cos, sin = rope_tables(jnp.concatenate(positions), hd)

        proj = lambda x, w, eq: jnp.einsum(eq, x, w, preferred_element_type=F32).astype(BF16)
        kv = proj(hidden, wkv, 'bld,de->ble')
        do = proj(d_out, wo, 'bld,ed->ble')
        q = proj(hidden, wq, 'bld,de->ble')
        o, dq, dkv = attention(q, do, kv, cos, sin, hd)
        dkv_back = lax.ppermute(dkv[:, local_len:], 'sp', [(d, d ^ 1) for d in range(n)])

        dkv = dkv[:, :local_len]
        dkv = jnp.concatenate([jnp.where(core == 0, dkv, dkv_back), jnp.where(core == 0, dkv_back, dkv)], axis=0)
        flat = lambda x: x.reshape(batch * local_len, -1)
        grad_wo, grad_wq, grad_wkv, attn_out, d_hidden = sum_all(flat(hidden), flat(d_out), flat(o), wo, flat(dq), wq, flat(dkv), wkv)
        attn_out, d_hidden = attn_out.reshape(hidden.shape), d_hidden.reshape(hidden.shape)
        return (attn_out, d_hidden, grad_wq.reshape(w_query.shape), grad_wkv[:hd].T, grad_wkv[hd:].T, grad_wo.reshape(w_out.shape))

    return jax.shard_map(local_step, mesh=mesh, in_specs=(seq_spec, seq_spec, rep_spec, rep_spec, rep_spec, rep_spec), out_specs=(seq_spec, seq_spec, rep_spec, rep_spec, rep_spec, rep_spec), check_vma=False)
```

```python
import functools

import jax
import jax.numpy as jnp
from jax import lax
from jax.experimental import pallas as pl
from jax.experimental.pallas import tpu as pltpu
from jax.sharding import PartitionSpec as P

F32 = jnp.float32
BF16 = jnp.bfloat16
NT = (((1,), (1,)), ((), ()))
NN = (((1,), (0,)), ((), ()))
TN = (((0,), (0,)), ((), ()))
LOG2E = 1.4426950408889634
CHIP_BLOCKS = ((0,), (0, 1), (0, 2, 3), (0, 1, 2, 3))


def dot(a, b, dims):
    return lax.dot_general(a, b, dims, preferred_element_type=F32)


def rope_tables(positions, head_dim):
    half_dim = head_dim // 2
    inv_freq = 10000.0 ** (-(jnp.arange(half_dim).astype(F32) * 2.0) / head_dim)
    angles = positions.astype(F32)[:, None] * inv_freq[None, :]
    return jnp.cos(angles), jnp.sin(angles)


def rotate(x, cos, sin, sign):
    half = x.shape[-1] // 2
    a, b = x[..., :half].astype(F32), x[..., half:].astype(F32)
    s = sin * sign
    return jnp.concatenate([a * cos - b * s, b * cos + a * s], axis=-1).astype(BF16)


def attn_step(blocks, heads, hd, scale, core, first, s, step, q_refs, do_refs, kv, k_rot, cos_ref, sin_ref, stage, slot, acc):
    rows = kv.shape[2]
    half_rows = rows // 2
    flip = core * half_rows
    pos = lambda t: jnp.where(t < half_rows, t + flip, t - flip)
    cos, sin = cos_ref[:rows], sin_ref[:rows]

    @pl.when(first)
    def _():
        for b in blocks:
            tab = slice(b * rows, (b + 1) * rows)
            acc[b, s] = jnp.zeros_like(acc[b, s])
            k_rot[b] = rotate(kv[b, s, :, :hd], cos_ref[tab], sin_ref[tab], 1.0)

    keep = pos(lax.broadcasted_iota(jnp.int32, (rows, rows), 0)) >= pos(lax.broadcasted_iota(jnp.int32, (rows, rows), 1))
    qs, dos, dss, pbs = [], [], [], []
    for h in range(heads):
        cols = slice(h * hd, (h + 1) * hd)
        wide = pl.ds(pl.multiple_of((step * heads + h) * hd, hd), hd)
        q = rotate(jnp.concatenate([q_refs[0][0, :, cols], q_refs[1][s, :, wide]], axis=0), cos, sin, 1.0)
        do = jnp.concatenate([do_refs[0][0, :, cols], do_refs[1][s, :, wide]], axis=0)
        sc = [dot(q, k_rot[b], NT) for b in blocks]
        sc[0] = jnp.where(keep, sc[0], -jnp.inf)
        m = functools.reduce(jnp.maximum, [jnp.max(t, axis=1, keepdims=True) for t in sc])
        e = [jnp.exp2((t - m) * (scale * LOG2E)) for t in sc]
        inv = 1.0 / functools.reduce(jnp.add, [jnp.sum(t, axis=1, keepdims=True) for t in e])
        p = [t * inv for t in e]
        pb = [t.astype(BF16) for t in p]
        o = functools.reduce(jnp.add, [dot(pb[i], kv[b, s, :, hd:], NN) for i, b in enumerate(blocks)]).astype(BF16)
        stage[slot, 0, 0, :, wide] = o[:half_rows]
        stage[slot, 0, 1, :, wide] = o[half_rows:]
        delta = jnp.sum(do.astype(F32) * o.astype(F32), axis=1, keepdims=True)
        ds = [(p[i] * (dot(do, kv[b, s, :, hd:], NT) - delta) * scale).astype(BF16) for i, b in enumerate(blocks)]
        dq = functools.reduce(jnp.add, [dot(ds[i], k_rot[b], NN) for i, b in enumerate(blocks)]).astype(BF16)
        dq = rotate(dq, cos, sin, -1.0)
        stage[slot, 1, 0, :, wide] = dq[:half_rows]
        stage[slot, 1, 1, :, wide] = dq[half_rows:]
        qs.append(q)
        dos.append(do)
        dss.append(ds)
        pbs.append(pb)
    q, do = jnp.concatenate(qs, axis=0), jnp.concatenate(dos, axis=0)
    for i, b in enumerate(blocks):
        dk = dot(jnp.concatenate([t[i] for t in dss], axis=0), q, TN)
        dv = dot(jnp.concatenate([t[i] for t in pbs], axis=0), do, TN)
        acc[b, s, :, :hd] += dk
        acc[b, s, :, hd:] += dv


MESH = pl.DeviceIdType.MESH
PIECE = 512


def remote(src, dst, sems, i, dev):
    return pltpu.make_async_remote_copy(src_ref=src, dst_ref=dst, send_sem=sems.at[0, i], recv_sem=sems.at[1, i], device_id=(dev,), device_id_type=MESH)


def sum_kernel(counts, *refs):
    ng = len(counts)
    hid_ref, dout_ref, o_ref, wo_ref, dq_ref, wq_ref, dkv_ref, wkv_ref = refs[:8]
    out_refs, (attn_out, d_hidden, dr) = refs[8:ng + 8], refs[ng + 8:ng + 11]
    h, dv, give, flip, r1, r2, xs, ws, xs2, ws2, tiles, dr_sem, mm_sem, tile_sem, keep_sem, d_sem, s1_sem, s2_sem, g1_sem, g2_sem, g3_sem = refs[ng + 11:]
    total = sum(counts)
    dev = lax.axis_index('sp')
    chip, core = dev // 2, dev % 2
    bits = (chip % 2, chip // 2)
    partner = dev + 1 - 2 * core
    across = (dev + 2 - 4 * bits[0], dev + 4 - 8 * bits[1])
    half, quarter, eighth, last = PIECE // 2, PIECE // 4, PIECE // 8, PIECE // 16

    barrier = pltpu.get_barrier_semaphore()
    for d in (partner,) + across:
        pl.semaphore_signal(barrier, inc=1, device_id=(d,), device_id_type=MESH)
    pl.semaphore_wait(barrier, 3)

    def rows(ref, start, size):
        return ref.at[pl.ds(pl.multiple_of(start, 32), size)]

    def each(body, which=range(ng)):
        base = 0
        for i, count in enumerate(counts):
            def step(p, carry, i=i, base=base):
                body(i, p, base + p)
                return carry
            if i in which:
                lax.fori_loop(0, count, step, 0)
            base += count

    def cross(s):
        return remote(give.at[s % 2], dr.at[s], d_sem, s, partner)

    def first(w, s):
        src = h.at[s, pl.ds(pl.multiple_of(w * quarter + (1 - bits[w]) * eighth, 32), eighth)]
        return remote(src, r1.at[w, s], s1_sem.at[w], s, across[w])

    def second(w, s):
        src = h.at[s, pl.ds(pl.multiple_of(w * quarter + bits[w] * eighth + (1 - bits[1 - w]) * last, 32), last)]
        return remote(src, r2.at[w, s], s2_sem.at[w], s, across[1 - w])

    def kept(w):
        return w * quarter + bits[w] * eighth

    def final(w):
        return kept(w) + bits[1 - w] * last

    def keep(w, i, p, s):
        return pltpu.make_async_copy(h.at[s, pl.ds(pl.multiple_of(final(w), 32), last)], rows(out_refs[i], p * PIECE + core * half + final(w), last), keep_sem.at[w, s])

    def share1(w, i, p, s):
        return remote(h.at[s, pl.ds(pl.multiple_of(final(w), 32), last)], rows(out_refs[i], p * PIECE + core * half + final(w), last), g1_sem.at[w], s, across[1 - w])

    def share2(w, i, p, s):
        here = rows(out_refs[i], p * PIECE + core * half + kept(w), eighth)
        return remote(here, here, g2_sem.at[w], s, across[w])

    def share3(i, p, s):
        here = rows(out_refs[i], p * PIECE + core * half, half)
        return remote(here, here, g3_sem, s, partner)

    def product_rows(left, right, start, put):
        cols = pl.ds(pl.multiple_of(start, half), half)

        @pl.loop(0, left.shape[0], step=half)
        def _(r):
            at = pl.ds(pl.multiple_of(r, half), half)
            flip[:, at] = left[at, cols].T

        @pl.loop(0, right.shape[1], step=512)
        def _(c):
            at = pl.ds(pl.multiple_of(c, 512), 512)
            put(at, dot(flip[...], right[:, at], NN))

    def phase1(left, right, i, p, s):
        @pl.when(s >= 2)
        def _():
            cross(s - 2).wait_send()

        def put_give(at, x):
            give[s % 2, :, at] = x

        def put_keep(at, x):
            h[s, :, at] = x
        product_rows(left, right, p * PIECE + (1 - core) * half, put_give)
        cross(s).start()
        product_rows(left, right, p * PIECE + core * half, put_keep)
        cross(s).wait_recv()
        fetch = pltpu.make_async_copy(dr.at[s], dv, dr_sem)
        fetch.start()
        fetch.wait()

        @pl.loop(0, half, step=32)
        def _(r):
            at = pl.ds(pl.multiple_of(r, 32), 32)
            h[s, at] += dv[at]
        for w in range(2):
            first(w, s).start()

    def phase2(i, p, s):
        for w in range(2):
            first(w, s).wait()
            at = pl.ds(pl.multiple_of(kept(w), 32), eighth)
            h[s, at] += r1[w, s]
            second(w, s).start()

    def phase3(i, p, s):
        for w in range(2):
            second(w, s).wait()
            at = pl.ds(pl.multiple_of(final(w), 32), last)
            h[s, at] += r2[w, s]
            share1(w, i, p, s).start()
            keep(w, i, p, s).start()

    def phase4(i, p, s):
        for w in range(2):
            share1(w, i, p, s).wait()
            keep(w, i, p, s).wait()
            share2(w, i, p, s).start()

    def phase5(i, p, s):
        for w in range(2):
            share2(w, i, p, s).wait()
        share3(i, p, s).start()

    def phase6(i, p, s):
        share3(i, p, s).wait()

    tm, tn = tiles.shape[1:]
    across_n = ws.shape[0] // tn
    n_tiles = xs.shape[0] // tm * across_n

    def bring(src, dst, k):
        return pltpu.make_async_copy(src, dst, mm_sem.at[k])

    def spill(out, t):
        at = (pl.ds(pl.multiple_of(t // across_n * tm, tm), tm), pl.ds(pl.multiple_of(t % across_n * tn, tn), tn))
        return pltpu.make_async_copy(tiles.at[t % 2], out.at[at], tile_sem.at[t % 2])

    def matmul(out, product):
        @pl.loop(0, n_tiles)
        def _(t):
            @pl.when(t >= 2)
            def _():
                spill(out, t - 2).wait()
            m, c = pl.ds(pl.multiple_of(t // across_n * tm, tm), tm), pl.ds(pl.multiple_of(t % across_n * tn, tn), tn)
            tiles[t % 2] = product(m, c).astype(BF16)
            spill(out, t).start()
        for t in (n_tiles - 2, n_tiles - 1):
            spill(out, t).wait()

    def forward(m, c):
        return dot(ws[m], xs[:, c], NN)

    def backward(m, c):
        return dot(ws[m], xs[c], NT) + dot(xs2[m], ws2[c], NT)

    def bring_all(*pairs):
        copies = [bring(src, dst, k) for k, (src, dst) in enumerate(pairs)]
        for copy in copies:
            copy.start()
        for copy in copies:
            copy.wait()

    bring_all((o_ref, xs), (dout_ref, ws))
    each(functools.partial(phase1, xs, ws), (0,))
    bring_all((hid_ref, xs), (dq_ref, ws), (dkv_ref, xs2), (wkv_ref, ws2))
    each(functools.partial(phase1, xs, ws), (1,))
    each(functools.partial(phase1, xs2, xs), (2,))
    for s in (total - 2, total - 1):
        cross(s).wait_send()
    bring_all((wq_ref, xs))
    each(phase2, (0,))
    matmul(d_hidden, backward)
    each(phase2, (1, 2))
    bring_all((o_ref, ws), (wo_ref, xs))
    each(phase3, (0,))
    matmul(attn_out, forward)
    each(phase3, (1, 2))
    for phase in (phase4, phase5, phase6):
        each(phase)


def sum_all(hidden, d_out, o, wo, dq, wq, dkv, wkv):
    grads = [(o.shape[1], d_out.shape[1]), (hidden.shape[1], dq.shape[1]), (dkv.shape[1], hidden.shape[1])]
    counts = tuple(g[0] // PIECE for g in grads)
    total = sum(counts)
    width = grads[0][1]
    dma = pltpu.SemaphoreType.DMA
    hbm = pl.BlockSpec(memory_space=pl.ANY)
    act = jax.ShapeDtypeStruct((o.shape[0], wo.shape[1]), BF16)
    res = pl.pallas_call(
        functools.partial(sum_kernel, counts),
        out_shape=[jax.ShapeDtypeStruct(g, F32) for g in grads] + [act, act, jax.ShapeDtypeStruct((total, PIECE // 2, width), F32)],
        in_specs=[hbm] * 8,
        out_specs=[hbm] * (len(grads) + 3),
        scratch_shapes=[
            pltpu.VMEM((total, PIECE // 2, width), F32),
            pltpu.VMEM((PIECE // 2, width), F32),
            pltpu.VMEM((2, PIECE // 2, width), F32),
            pltpu.VMEM((PIECE // 2, o.shape[0]), BF16),
            pltpu.VMEM((2, total, PIECE // 8, width), F32),
            pltpu.VMEM((2, total, PIECE // 16, width), F32),
            pltpu.VMEM(o.shape, BF16), pltpu.VMEM(wo.shape, BF16),
            pltpu.VMEM(dkv.shape, BF16), pltpu.VMEM(wkv.shape, BF16),
            pltpu.VMEM((2, 512, 256), BF16),
            dma, dma((4,)), dma((2,)), dma((2, total)), dma((2, total)),
            dma((2, 2, total)), dma((2, 2, total)), dma((2, 2, total)), dma((2, 2, total)), dma((2, total)),
        ],
        compiler_params=pltpu.CompilerParams(collective_id=1, has_side_effects=True, vmem_limit_bytes=67 * 1000 * 1000),
        name="sum_all",
    )(hidden, d_out, o, wo, dq, wq, dkv, wkv)
    return res[:-1]


def attn_kernel(heads, hd, lag, q_mine, do_mine, q_all, do_all, kv_all, cos_ref, sin_ref, o_out, dq_out, dkv_out,
                kv, k_rot, q_in, do_in, stage, acc, relay, got, kv_mine_sem, pair_sem, kv_sem, pass_sem, in_sem, keep_sem, give_sem, one_sem, two_sem):
    s, step = pl.program_id(0), pl.program_id(1)
    steps = pl.num_programs(1)
    ns, rows = kv.shape[1], kv.shape[2]
    half_rows = rows // 2
    dev = lax.axis_index('sp')
    chip, core = dev // 2, dev % 2
    bit_x, bit_y = chip % 2, chip // 2
    partner = dev + 1 - 2 * core
    dev_x, dev_y = dev + 2 - 4 * bit_x, dev + 4 - 8 * bit_y
    dev_d = dev_x + 4 - 8 * bit_y
    mine, yours = core * ns, (1 - core) * ns
    slot = s % 2

    def give_kv(b, i):
        return remote(kv.at[0, i], kv.at[b, i], kv_sem.at[b - 1], i, (dev_x, dev_y, dev_d)[b - 1])

    def give_in(i, k):
        return remote((q_all, do_all)[k].at[yours + i], (q_in, do_in)[k].at[i], in_sem.at[k], i, partner)

    up = ((bit_x == 0) | (chip == 1), bit_y == 0, chip == 0)
    down = (bit_x == 1, bit_y == 1, chip == 3)

    def pass_on(i):
        return remote(kv.at[1, i], kv.at[3, i], pass_sem, i, dev_y)

    def pair():
        return remote(kv_all.at[pl.ds(yours, ns)], kv.at[0, :, pl.ds(half_rows, half_rows)], pair_sem, 0, partner)

    def own():
        return pltpu.make_async_copy(kv_all.at[pl.ds(mine, ns)], kv.at[0, :, pl.ds(0, half_rows)], kv_mine_sem)

    @pl.when((s == 0) & (step == 0))
    def _():
        barrier = pltpu.get_barrier_semaphore()
        for d in (partner, dev_x, dev_y, dev_d):
            pl.semaphore_signal(barrier, inc=1, device_id=(d,), device_id_type=MESH)
        pl.semaphore_wait(barrier, 4)
        pair().start()
        own().start()
        for k in range(2):
            give_in(0, k).start()
        own().wait()
        pair().wait()

        @pl.loop(0, ns)
        def _(i):
            for b, turn in ((1, up[0]), (2, chip == 1), (3, up[2])):
                @pl.when(turn)
                def _():
                    give_kv(b, i).start()

            @pl.when(i > 0)
            def _():
                for k in range(2):
                    give_in(i, k).start()

        @pl.when(chip == 0)
        def _():
            @pl.loop(0, ns)
            def _(i):
                give_kv(2, i).start()
                give_kv(1, i).wait_recv()
                pass_on(i).start()

    def keep(i, k):
        return pltpu.make_async_copy(stage.at[i % 2, k, 0], (o_out, dq_out)[k].at[mine + i], keep_sem.at[k, i % 2])

    def give(i, k):
        return remote(stage.at[i % 2, k, 1], (o_out, dq_out)[k].at[mine + i], give_sem.at[k], i, partner)

    @pl.when(step == 0)
    def _():
        for k in range(2):
            give_in(s, k).wait()
        for b in (1, 2, 3):
            @pl.when(down[b - 1])
            def _():
                give_kv(b, s).wait_recv()

        @pl.when(chip == 2)
        def _():
            pass_on(s).wait_recv()

        @pl.when(s >= 2)
        def _():
            for k in range(2):
                keep(s - 2, k).wait()
                give(s - 2, k).wait_send()

    first = step == 0
    for c, blocks in enumerate(CHIP_BLOCKS):
        @pl.when(chip == c)
        def _():
            attn_step(blocks, heads, hd, hd ** -0.5, core, first, s, step, (q_mine, q_in), (do_mine, do_in), kv, k_rot, cos_ref, sin_ref, stage, slot, acc)

    def one(i, w):
        return remote(acc.at[3, i], relay.at[i], one_sem, i, (dev_x, dev_y)[w])

    def two(i, w):
        return remote(acc.at[1 + w, i], got.at[w, i], two_sem.at[w], i, (dev_x, dev_y)[w])

    def send_one(i):
        for w in range(2):
            @pl.when((bit_y == 1) & (i % 2 == w))
            def _():
                one(i, w).start()

    def send_two(i):
        even = i % 2 == 0
        @pl.when(even & (bit_y == 1))
        def _():
            one(i, 0).wait_recv()
            acc[2, i] += relay[i]

        @pl.when(jnp.logical_not(even) & (chip == 1))
        def _():
            one(i, 1).wait_recv()
            acc[1, i] += relay[i]

        @pl.when(jnp.logical_not(even) & (chip == 0))
        def _():
            one(i, 1).wait_recv()
            acc[1, i] = relay[i]

        @pl.when((bit_x == 1) | ((chip == 0) & jnp.logical_not(even)))
        def _():
            two(i, 0).start()

        @pl.when(bit_y == 1)
        def _():
            two(i, 1).start()

    def finish(i):
        even = i % 2 == 0

        @pl.when((bit_x == 0) | ((chip == 1) & jnp.logical_not(even)))
        def _():
            two(i, 0).wait_recv()
            acc[0, i] += got[0, i]

        @pl.when(bit_y == 0)
        def _():
            two(i, 1).wait_recv()
            acc[0, i] += got[1, i]
        total = acc[0, i].astype(BF16)
        dkv_out[i, :, :hd] = rotate(total[:, :hd], cos_ref[:rows], sin_ref[:rows], -1.0)
        dkv_out[i, :, hd:] = total[:, hd:]

    @pl.when(step == steps - 1)
    def _():
        for k in range(2):
            keep(s, k).start()
            give(s, k).start()
        send_one(s)

        @pl.when(s >= lag)
        def _():
            send_two(s - lag)

    @pl.when((s == ns - 1) & (step == steps - 1))
    def _():
        @pl.loop(ns - lag, ns)
        def _(i):
            send_two(i)

        @pl.loop(0, ns)
        def _(i):
            finish(i)
            for k in range(2):
                give(i, k).wait_recv()
            for b in (1, 2, 3):
                @pl.when(up[b - 1])
                def _():
                    give_kv(b, i).wait_send()

            @pl.when(chip == 0)
            def _():
                pass_on(i).wait_send()
            for w in range(2):
                @pl.when((bit_y == 1) & (i % 2 == w))
                def _():
                    one(i, w).wait_send()

            @pl.when((bit_x == 1) | ((chip == 0) & (i % 2 == 1)))
            def _():
                two(i, 0).wait_send()

            @pl.when(bit_y == 1)
            def _():
                two(i, 1).wait_send()
        for i in (ns - 2, ns - 1):
            for k in range(2):
                keep(i, k).wait()
                give(i, k).wait_send()


def attention(q, do, kv, cos, sin, hd, heads=2, lag=2):
    batch, half_rows, width = q.shape
    ns, rows = batch // 2, 2 * half_rows
    mine = pl.BlockSpec((1, half_rows, heads * hd), lambda s, h: (lax.axis_index('sp') % 2 * ns + s, 0, h))
    tab = pl.BlockSpec((4 * rows, hd // 2), lambda s, h: (0, 0))
    hbm = pl.BlockSpec(memory_space=pl.ANY)
    act = jax.ShapeDtypeStruct(q.shape, BF16)
    dma = pltpu.SemaphoreType.DMA
    return pl.pallas_call(
        functools.partial(attn_kernel, heads, hd, lag),
        grid=(ns, width // (heads * hd)),
        in_specs=[mine, mine, hbm, hbm, hbm, tab, tab],
        out_specs=[hbm, hbm, pl.BlockSpec((ns, rows, 2 * hd), lambda s, h: (0, 0, 0))],
        out_shape=[act, act, jax.ShapeDtypeStruct((ns, rows, 2 * hd), BF16)],
        scratch_shapes=[
            pltpu.VMEM((4, ns, rows, 2 * hd), BF16),
            pltpu.VMEM((4, rows, hd), BF16),
            pltpu.VMEM((ns, half_rows, width), BF16),
            pltpu.VMEM((ns, half_rows, width), BF16),
            pltpu.VMEM((2, 2, 2, half_rows, width), BF16),
            pltpu.VMEM((4, ns, rows, 2 * hd), F32),
            pltpu.VMEM((ns, rows, 2 * hd), F32),
            pltpu.VMEM((2, ns, rows, 2 * hd), F32),
            dma, dma((2, 1)), dma((3, 2, ns)), dma((2, ns)), dma((2, 2, ns)), dma((2, 2)), dma((2, 2, ns)), dma((2, ns)), dma((2, 2, ns)),
        ],
        compiler_params=pltpu.CompilerParams(dimension_semantics=("arbitrary", "arbitrary"), collective_id=2, has_side_effects=True, vmem_limit_bytes=66 * 1000 * 1000),
        cost_estimate=pl.CostEstimate(flops=6 * 2 * ns * rows * width * rows * 4, bytes_accessed=100 * 1024 * 1024, transcendentals=0),
        name="attention",
    )(q, do, q, do, kv, cos, sin)


def place_kernel(gwo, gwq, gwkv, a, d, wo, wq, wk, wv, a_out, d_out):
    hd = wk.shape[1]
    wo[...] = gwo[...]
    for h in range(wq.shape[1]):
        wq[:, h, :] = gwq[:, h * hd:(h + 1) * hd]
    t = gwkv[...].T
    wk[...] = t[:, :hd]
    wv[...] = t[:, hd:]
    a_out[...] = a[...]
    d_out[...] = d[...]


def place(gwo, gwq, gwkv, a, d, heads):
    m, n = gwq.shape
    hd = n // heads
    tile = 128
    rows = lambda w: pl.BlockSpec((tile, w), lambda i: (i, 0))
    return pl.pallas_call(
        place_kernel,
        grid=(m // tile,),
        in_specs=[rows(n), rows(n), pl.BlockSpec((2 * hd, tile), lambda i: (0, i)), rows(a.shape[1]), rows(d.shape[1])],
        out_specs=[rows(n), pl.BlockSpec((tile, heads, hd), lambda i: (i, 0, 0)), rows(hd), rows(hd), rows(a.shape[1]), rows(d.shape[1])],
        out_shape=[jax.ShapeDtypeStruct((m, n), F32), jax.ShapeDtypeStruct((m, heads, hd), F32), jax.ShapeDtypeStruct((m, hd), F32), jax.ShapeDtypeStruct((m, hd), F32), jax.ShapeDtypeStruct(a.shape, BF16), jax.ShapeDtypeStruct(d.shape, BF16)],
        compiler_params=pltpu.CompilerParams(dimension_semantics=("arbitrary",), vmem_limit_bytes=40 * 1000 * 1000),
        name="place",
    )(gwo, gwq, gwkv, a, d)


def solution(mesh):
    n = mesh.shape['sp']
    seq_spec = P(None, 'sp', None)
    rep_spec = P()

    def local_step(hidden, d_out, w_query, w_key, w_value, w_out):
        batch, local_len, width = hidden.shape
        hd = w_key.shape[1]
        qw = w_query.shape[1] * hd
        dev = lax.axis_index('sp')
        core = dev % 2
        wq = lax.optimization_barrier(w_query.reshape(width, qw))
        wo = w_out.reshape(qw, width)
        wkv = jnp.concatenate([w_key, w_value], axis=1)

        offset = jnp.arange(local_len)
        positions = [((dev ^ (2 * b)) ^ c) * local_len + offset for b in range(4) for c in range(2)]
        cos, sin = rope_tables(jnp.concatenate(positions), hd)

        proj = lambda x, w, eq: jnp.einsum(eq, x, w, preferred_element_type=F32).astype(BF16)
        kv = proj(hidden, wkv, 'bld,de->ble')
        do = proj(d_out, wo, 'bld,ed->ble')
        q = proj(hidden, wq, 'bld,de->ble')
        o, dq, dkv = attention(q, do, kv, cos, sin, hd)
        dkv_back = lax.ppermute(dkv[:, local_len:], 'sp', [(d, d ^ 1) for d in range(n)])

        dkv = dkv[:, :local_len]
        dkv = jnp.concatenate([jnp.where(core == 0, dkv, dkv_back), jnp.where(core == 0, dkv_back, dkv)], axis=0)
        flat = lambda x: x.reshape(batch * local_len, -1)
        grad_wo, grad_wq, grad_wkv, attn_out, d_hidden = sum_all(flat(hidden), flat(d_out), flat(o), wo, flat(dq), wq, flat(dkv), wkv)
        grad_wo, grad_wq, grad_wk, grad_wv, attn_out, d_hidden = place(grad_wo, grad_wq, grad_wkv, attn_out, d_hidden, w_query.shape[1])
        return (attn_out.reshape(hidden.shape), d_hidden.reshape(hidden.shape), grad_wq, grad_wk, grad_wv, grad_wo.reshape(w_out.shape))

    return jax.shard_map(local_step, mesh=mesh, in_specs=(seq_spec, seq_spec, rep_spec, rep_spec, rep_spec, rep_spec), out_specs=(seq_spec, seq_spec, rep_spec, rep_spec, rep_spec, rep_spec), check_vma=False)
```

```python
import functools

import jax
import jax.numpy as jnp
from jax import lax
from jax.experimental import pallas as pl
from jax.experimental.pallas import tpu as pltpu
from jax.sharding import PartitionSpec as P

F32 = jnp.float32
BF16 = jnp.bfloat16
NT = (((1,), (1,)), ((), ()))
NN = (((1,), (0,)), ((), ()))
TN = (((0,), (0,)), ((), ()))
LOG2E = 1.4426950408889634
CHIP_BLOCKS = ((0,), (0, 1), (0, 2, 3), (0, 1, 2, 3))


def dot(a, b, dims):
    return lax.dot_general(a, b, dims, preferred_element_type=F32)


def rope_tables(positions, head_dim):
    half_dim = head_dim // 2
    inv_freq = 10000.0 ** (-(jnp.arange(half_dim).astype(F32) * 2.0) / head_dim)
    angles = positions.astype(F32)[:, None] * inv_freq[None, :]
    return jnp.cos(angles), jnp.sin(angles)


def rotate(x, cos, sin, sign):
    half = x.shape[-1] // 2
    a, b = x[..., :half].astype(F32), x[..., half:].astype(F32)
    s = sin * sign
    return jnp.concatenate([a * cos - b * s, b * cos + a * s], axis=-1).astype(BF16)


def attn_step(blocks, heads, hd, scale, core, first, s, step, q_refs, do_refs, kv, k_rot, cos_ref, sin_ref, stage, slot, acc):
    rows = kv.shape[2]
    half_rows = rows // 2
    flip = core * half_rows
    pos = lambda t: jnp.where(t < half_rows, t + flip, t - flip)
    cos, sin = cos_ref[:rows], sin_ref[:rows]

    @pl.when(first)
    def _():
        for b in blocks:
            tab = slice(b * rows, (b + 1) * rows)
            acc[b, s] = jnp.zeros_like(acc[b, s])
            k_rot[b] = rotate(kv[b, s, :, :hd], cos_ref[tab], sin_ref[tab], 1.0)

    keep = pos(lax.broadcasted_iota(jnp.int32, (rows, rows), 0)) >= pos(lax.broadcasted_iota(jnp.int32, (rows, rows), 1))
    qs, dos, dss, pbs = [], [], [], []
    for h in range(heads):
        cols = slice(h * hd, (h + 1) * hd)
        wide = pl.ds(pl.multiple_of((step * heads + h) * hd, hd), hd)
        q = rotate(jnp.concatenate([q_refs[0][0, :, cols], q_refs[1][s, :, wide]], axis=0), cos, sin, 1.0)
        do = jnp.concatenate([do_refs[0][0, :, cols], do_refs[1][s, :, wide]], axis=0)
        sc = [dot(q, k_rot[b], NT) for b in blocks]
        sc[0] = jnp.where(keep, sc[0], -jnp.inf)
        m = functools.reduce(jnp.maximum, [jnp.max(t, axis=1, keepdims=True) for t in sc])
        e = [jnp.exp2((t - m) * (scale * LOG2E)) for t in sc]
        inv = 1.0 / functools.reduce(jnp.add, [jnp.sum(t, axis=1, keepdims=True) for t in e])
        p = [t * inv for t in e]
        pb = [t.astype(BF16) for t in p]
        o = functools.reduce(jnp.add, [dot(pb[i], kv[b, s, :, hd:], NN) for i, b in enumerate(blocks)]).astype(BF16)
        stage[slot, 0, 0, :, wide] = o[:half_rows]
        stage[slot, 0, 1, :, wide] = o[half_rows:]
        delta = jnp.sum(do.astype(F32) * o.astype(F32), axis=1, keepdims=True)
        ds = [(p[i] * (dot(do, kv[b, s, :, hd:], NT) - delta) * scale).astype(BF16) for i, b in enumerate(blocks)]
        dq = functools.reduce(jnp.add, [dot(ds[i], k_rot[b], NN) for i, b in enumerate(blocks)]).astype(BF16)
        dq = rotate(dq, cos, sin, -1.0)
        stage[slot, 1, 0, :, wide] = dq[:half_rows]
        stage[slot, 1, 1, :, wide] = dq[half_rows:]
        qs.append(q)
        dos.append(do)
        dss.append(ds)
        pbs.append(pb)
    q, do = jnp.concatenate(qs, axis=0), jnp.concatenate(dos, axis=0)
    for i, b in enumerate(blocks):
        dk = dot(jnp.concatenate([t[i] for t in dss], axis=0), q, TN)
        dv = dot(jnp.concatenate([t[i] for t in pbs], axis=0), do, TN)
        acc[b, s, :, :hd] += dk
        acc[b, s, :, hd:] += dv


MESH = pl.DeviceIdType.MESH
PIECE = 512


def remote(src, dst, sems, i, dev):
    return pltpu.make_async_remote_copy(src_ref=src, dst_ref=dst, send_sem=sems.at[0, i], recv_sem=sems.at[1, i], device_id=(dev,), device_id_type=MESH)


def sum_kernel(counts, *refs):
    ng = len(counts)
    hid_ref, dout_ref, o_ref, wo_ref, dq_ref, wq_ref, dkv_ref, wkv_ref = refs[:8]
    out_refs, (attn_out, d_hidden, dr) = refs[8:ng + 8], refs[ng + 8:ng + 11]
    h, dv, give, flip, r1, r2, xs, ws, xs2, ws2, tiles, early_sem, dr_sem, mm_sem, tile_sem, keep_sem, d_sem, s1_sem, s2_sem, g1_sem, g2_sem, g3_sem = refs[ng + 11:]
    total = sum(counts)
    dev = lax.axis_index('sp')
    chip, core = dev // 2, dev % 2
    bits = (chip % 2, chip // 2)
    partner = dev + 1 - 2 * core
    across = (dev + 2 - 4 * bits[0], dev + 4 - 8 * bits[1])
    half, quarter, eighth, last = PIECE // 2, PIECE // 4, PIECE // 8, PIECE // 16

    barrier = pltpu.get_barrier_semaphore()
    for d in (partner,) + across:
        pl.semaphore_signal(barrier, inc=1, device_id=(d,), device_id_type=MESH)
    pl.semaphore_wait(barrier, 3)

    def rows(ref, start, size):
        return ref.at[pl.ds(pl.multiple_of(start, 32), size)]

    def each(body, which=range(ng), start=0):
        base = 0
        for i, count in enumerate(counts):
            def step(p, carry, i=i, base=base):
                body(i, p, base + p)
                return carry
            if i in which:
                lax.fori_loop(start, count, step, 0)
            base += count

    def cross(s):
        return remote(give.at[s % 2], dr.at[s], d_sem, s, partner)

    def first(w, s):
        src = h.at[s, pl.ds(pl.multiple_of(w * quarter + (1 - bits[w]) * eighth, 32), eighth)]
        return remote(src, r1.at[w, s], s1_sem.at[w], s, across[w])

    def second(w, s):
        src = h.at[s, pl.ds(pl.multiple_of(w * quarter + bits[w] * eighth + (1 - bits[1 - w]) * last, 32), last)]
        return remote(src, r2.at[w, s], s2_sem.at[w], s, across[1 - w])

    def kept(w):
        return w * quarter + bits[w] * eighth

    def final(w):
        return kept(w) + bits[1 - w] * last

    def keep(w, i, p, s):
        return pltpu.make_async_copy(h.at[s, pl.ds(pl.multiple_of(final(w), 32), last)], rows(out_refs[i], p * PIECE + core * half + final(w), last), keep_sem.at[w, s])

    def share1(w, i, p, s):
        return remote(h.at[s, pl.ds(pl.multiple_of(final(w), 32), last)], rows(out_refs[i], p * PIECE + core * half + final(w), last), g1_sem.at[w], s, across[1 - w])

    def share2(w, i, p, s):
        here = rows(out_refs[i], p * PIECE + core * half + kept(w), eighth)
        return remote(here, here, g2_sem.at[w], s, across[w])

    def share3(i, p, s):
        here = rows(out_refs[i], p * PIECE + core * half, half)
        return remote(here, here, g3_sem, s, partner)

    def product_rows(left, right, start, put):
        cols = pl.ds(pl.multiple_of(start, half), half)

        @pl.loop(0, left.shape[0], step=half)
        def _(r):
            at = pl.ds(pl.multiple_of(r, half), half)
            flip[:, at] = left[at, cols].T

        @pl.loop(0, right.shape[1], step=512)
        def _(c):
            at = pl.ds(pl.multiple_of(c, 512), 512)
            put(at, dot(flip[...], right[:, at], NN))

    def phase1(left, right, i, p, s):
        @pl.when(s >= 2)
        def _():
            cross(s - 2).wait_send()

        def put_give(at, x):
            give[s % 2, :, at] = x

        def put_keep(at, x):
            h[s, :, at] = x
        product_rows(left, right, p * PIECE + (1 - core) * half, put_give)
        cross(s).start()
        product_rows(left, right, p * PIECE + core * half, put_keep)
        cross(s).wait_recv()
        fetch = pltpu.make_async_copy(dr.at[s], dv, dr_sem)
        fetch.start()
        fetch.wait()

        @pl.loop(0, half, step=32)
        def _(r):
            at = pl.ds(pl.multiple_of(r, 32), 32)
            h[s, at] += dv[at]
        for w in range(2):
            first(w, s).start()

    def phase2(i, p, s):
        for w in range(2):
            first(w, s).wait()
            at = pl.ds(pl.multiple_of(kept(w), 32), eighth)
            h[s, at] += r1[w, s]
            second(w, s).start()

    def phase3(i, p, s):
        for w in range(2):
            second(w, s).wait()
            at = pl.ds(pl.multiple_of(final(w), 32), last)
            h[s, at] += r2[w, s]
            share1(w, i, p, s).start()
            keep(w, i, p, s).start()

    def phase4(i, p, s):
        for w in range(2):
            share1(w, i, p, s).wait()
            keep(w, i, p, s).wait()
            share2(w, i, p, s).start()

    def phase5(i, p, s):
        for w in range(2):
            share2(w, i, p, s).wait()
        share3(i, p, s).start()

    def phase6(i, p, s):
        share3(i, p, s).wait()

    tm, tn = tiles.shape[1:]
    across_n = ws.shape[0] // tn
    n_tiles = xs.shape[0] // tm * across_n

    def bring(src, dst, k):
        return pltpu.make_async_copy(src, dst, mm_sem.at[k])

    def spill(out, t):
        at = (pl.ds(pl.multiple_of(t // across_n * tm, tm), tm), pl.ds(pl.multiple_of(t % across_n * tn, tn), tn))
        return pltpu.make_async_copy(tiles.at[t % 2], out.at[at], tile_sem.at[t % 2])

    def matmul(out, product):
        @pl.loop(0, n_tiles)
        def _(t):
            @pl.when(t >= 2)
            def _():
                spill(out, t - 2).wait()
            m, c = pl.ds(pl.multiple_of(t // across_n * tm, tm), tm), pl.ds(pl.multiple_of(t % across_n * tn, tn), tn)
            tiles[t % 2] = product(m, c).astype(BF16)
            spill(out, t).start()
        for t in (n_tiles - 2, n_tiles - 1):
            spill(out, t).wait()

    def forward(m, c):
        return dot(ws[m], xs[:, c], NN)

    def backward(m, c):
        return dot(ws[m], xs[c], NT) + dot(xs2[m], ws2[c], NT)

    def bring_all(*pairs):
        copies = [bring(src, dst, k) for k, (src, dst) in enumerate(pairs)]
        for copy in copies:
            copy.start()
        for copy in copies:
            copy.wait()

    blocks = [pl.ds(PIECE * k, PIECE) for k in range(counts[0])]
    early = [pltpu.make_async_copy(src.at[:, at], dst.at[:, at], early_sem.at[g, k]) for k, at in enumerate(blocks) for g, (src, dst) in enumerate(((o_ref, xs), (dout_ref, ws)))]
    for copy in early:
        copy.start()
    early[0].wait()
    for copy in early[1::2]:
        copy.wait()
    phase1(xs, ws, 0, 0, 0)
    for copy in early[2::2]:
        copy.wait()
    each(functools.partial(phase1, xs, ws), (0,), 1)
    bring_all((hid_ref, xs), (dq_ref, ws), (dkv_ref, xs2), (wkv_ref, ws2))
    each(functools.partial(phase1, xs, ws), (1,))
    each(functools.partial(phase1, xs2, xs), (2,))
    for s in (total - 2, total - 1):
        cross(s).wait_send()
    bring_all((wq_ref, xs))
    each(phase2, (0,))
    matmul(d_hidden, backward)
    each(phase2, (1, 2))
    bring_all((o_ref, ws), (wo_ref, xs))
    each(phase3, (0,))
    matmul(attn_out, forward)
    each(phase3, (1, 2))
    for phase in (phase4, phase5, phase6):
        each(phase)


def sum_all(hidden, d_out, o, wo, dq, wq, dkv, wkv):
    grads = [(o.shape[1], d_out.shape[1]), (hidden.shape[1], dq.shape[1]), (dkv.shape[1], hidden.shape[1])]
    counts = tuple(g[0] // PIECE for g in grads)
    total = sum(counts)
    width = grads[0][1]
    dma = pltpu.SemaphoreType.DMA
    hbm = pl.BlockSpec(memory_space=pl.ANY)
    act = jax.ShapeDtypeStruct((o.shape[0], wo.shape[1]), BF16)
    res = pl.pallas_call(
        functools.partial(sum_kernel, counts),
        out_shape=[jax.ShapeDtypeStruct(g, F32) for g in grads] + [act, act, jax.ShapeDtypeStruct((total, PIECE // 2, width), F32)],
        in_specs=[hbm] * 8,
        out_specs=[hbm] * (len(grads) + 3),
        scratch_shapes=[
            pltpu.VMEM((total, PIECE // 2, width), F32),
            pltpu.VMEM((PIECE // 2, width), F32),
            pltpu.VMEM((2, PIECE // 2, width), F32),
            pltpu.VMEM((PIECE // 2, o.shape[0]), BF16),
            pltpu.VMEM((2, total, PIECE // 8, width), F32),
            pltpu.VMEM((2, total, PIECE // 16, width), F32),
            pltpu.VMEM(o.shape, BF16), pltpu.VMEM(wo.shape, BF16),
            pltpu.VMEM(dkv.shape, BF16), pltpu.VMEM(wkv.shape, BF16),
            pltpu.VMEM((2, 512, 256), BF16),
            dma((2, counts[0])), dma, dma((4,)), dma((2,)), dma((2, total)), dma((2, total)),
            dma((2, 2, total)), dma((2, 2, total)), dma((2, 2, total)), dma((2, 2, total)), dma((2, total)),
        ],
        compiler_params=pltpu.CompilerParams(collective_id=1, has_side_effects=True, vmem_limit_bytes=67 * 1000 * 1000),
        name="sum_all",
    )(hidden, d_out, o, wo, dq, wq, dkv, wkv)
    return res[:-1]


def attn_kernel(heads, hd, lag, q_mine, do_mine, q_all, do_all, kv_all, cos_ref, sin_ref, o_out, dq_out, dkv_out,
                kv, k_rot, q_in, do_in, stage, acc, relay, got, dkv, kv_mine_sem, pair_sem, kv_sem, pass_sem, in_sem, keep_sem, give_sem, one_sem, two_sem, home_sem, back_sem):
    s, step = pl.program_id(0), pl.program_id(1)
    steps = pl.num_programs(1)
    ns, rows = kv.shape[1], kv.shape[2]
    half_rows = rows // 2
    dev = lax.axis_index('sp')
    chip, core = dev // 2, dev % 2
    bit_x, bit_y = chip % 2, chip // 2
    partner = dev + 1 - 2 * core
    dev_x, dev_y = dev + 2 - 4 * bit_x, dev + 4 - 8 * bit_y
    dev_d = dev_x + 4 - 8 * bit_y
    mine, yours = core * ns, (1 - core) * ns
    slot = s % 2

    def give_kv(b, i):
        return remote(kv.at[0, i], kv.at[b, i], kv_sem.at[b - 1], i, (dev_x, dev_y, dev_d)[b - 1])

    def give_in(i, k):
        return remote((q_all, do_all)[k].at[yours + i], (q_in, do_in)[k].at[i], in_sem.at[k], i, partner)

    up = ((bit_x == 0) | (chip == 1), bit_y == 0, chip == 0)
    down = (bit_x == 1, bit_y == 1, chip == 3)

    def pass_on(i):
        return remote(kv.at[1, i], kv.at[3, i], pass_sem, i, dev_y)

    def pair():
        return remote(kv_all.at[pl.ds(yours, ns)], kv.at[0, :, pl.ds(half_rows, half_rows)], pair_sem, 0, partner)

    def own():
        return pltpu.make_async_copy(kv_all.at[pl.ds(mine, ns)], kv.at[0, :, pl.ds(0, half_rows)], kv_mine_sem)

    @pl.when((s == 0) & (step == 0))
    def _():
        barrier = pltpu.get_barrier_semaphore()
        for d in (partner, dev_x, dev_y, dev_d):
            pl.semaphore_signal(barrier, inc=1, device_id=(d,), device_id_type=MESH)
        pl.semaphore_wait(barrier, 4)
        pair().start()
        own().start()
        for k in range(2):
            give_in(0, k).start()
        own().wait()
        pair().wait()

        @pl.loop(0, ns)
        def _(i):
            for b, turn in ((1, up[0]), (2, chip == 1), (3, up[2])):
                @pl.when(turn)
                def _():
                    give_kv(b, i).start()

            @pl.when(i > 0)
            def _():
                for k in range(2):
                    give_in(i, k).start()

        @pl.when(chip == 0)
        def _():
            @pl.loop(0, ns)
            def _(i):
                give_kv(2, i).start()
                give_kv(1, i).wait_recv()
                pass_on(i).start()

    def keep(i, k):
        return pltpu.make_async_copy(stage.at[i % 2, k, 0], (o_out, dq_out)[k].at[mine + i], keep_sem.at[k, i % 2])

    def give(i, k):
        return remote(stage.at[i % 2, k, 1], (o_out, dq_out)[k].at[mine + i], give_sem.at[k], i, partner)

    @pl.when(step == 0)
    def _():
        for k in range(2):
            give_in(s, k).wait()
        for b in (1, 2, 3):
            @pl.when(down[b - 1])
            def _():
                give_kv(b, s).wait_recv()

        @pl.when(chip == 2)
        def _():
            pass_on(s).wait_recv()

        @pl.when(s >= 2)
        def _():
            for k in range(2):
                keep(s - 2, k).wait()
                give(s - 2, k).wait_send()

    first = step == 0
    for c, blocks in enumerate(CHIP_BLOCKS):
        @pl.when(chip == c)
        def _():
            attn_step(blocks, heads, hd, hd ** -0.5, core, first, s, step, (q_mine, q_in), (do_mine, do_in), kv, k_rot, cos_ref, sin_ref, stage, slot, acc)

    def one(i, w):
        return remote(acc.at[3, i], relay.at[i], one_sem, i, (dev_x, dev_y)[w])

    def two(i, w):
        return remote(acc.at[1 + w, i], got.at[w, i], two_sem.at[w], i, (dev_x, dev_y)[w])

    def send_one(i):
        for w in range(2):
            @pl.when((bit_y == 1) & (i % 2 == w))
            def _():
                one(i, w).start()

    def send_two(i):
        even = i % 2 == 0
        @pl.when(even & (bit_y == 1))
        def _():
            one(i, 0).wait_recv()
            acc[2, i] += relay[i]

        @pl.when(jnp.logical_not(even) & (chip == 1))
        def _():
            one(i, 1).wait_recv()
            acc[1, i] += relay[i]

        @pl.when(jnp.logical_not(even) & (chip == 0))
        def _():
            one(i, 1).wait_recv()
            acc[1, i] = relay[i]

        @pl.when((bit_x == 1) | ((chip == 0) & jnp.logical_not(even)))
        def _():
            two(i, 0).start()

        @pl.when(bit_y == 1)
        def _():
            two(i, 1).start()

    def finish(i):
        even = i % 2 == 0

        @pl.when((bit_x == 0) | ((chip == 1) & jnp.logical_not(even)))
        def _():
            two(i, 0).wait_recv()
            acc[0, i] += got[0, i]

        @pl.when(bit_y == 0)
        def _():
            two(i, 1).wait_recv()
            acc[0, i] += got[1, i]
        total = acc[0, i].astype(BF16)
        dkv[i, :, :hd] = rotate(total[:, :hd], cos_ref[:rows], sin_ref[:rows], -1.0)
        dkv[i, :, hd:] = total[:, hd:]
        home(i).start()
        back(i).start()

    def home(i):
        return pltpu.make_async_copy(dkv.at[i, pl.ds(0, half_rows)], dkv_out.at[mine + i], home_sem.at[i])

    def back(i):
        return remote(dkv.at[i, pl.ds(half_rows, half_rows)], dkv_out.at[mine + i], back_sem, i, partner)

    @pl.when(step == steps - 1)
    def _():
        for k in range(2):
            keep(s, k).start()
            give(s, k).start()
        send_one(s)

        @pl.when(s >= lag)
        def _():
            send_two(s - lag)

    @pl.when((s == ns - 1) & (step == steps - 1))
    def _():
        @pl.loop(ns - lag, ns)
        def _(i):
            send_two(i)

        @pl.loop(0, ns)
        def _(i):
            finish(i)
            for k in range(2):
                give(i, k).wait_recv()
            for b in (1, 2, 3):
                @pl.when(up[b - 1])
                def _():
                    give_kv(b, i).wait_send()

            @pl.when(chip == 0)
            def _():
                pass_on(i).wait_send()
            for w in range(2):
                @pl.when((bit_y == 1) & (i % 2 == w))
                def _():
                    one(i, w).wait_send()

            @pl.when((bit_x == 1) | ((chip == 0) & (i % 2 == 1)))
            def _():
                two(i, 0).wait_send()

            @pl.when(bit_y == 1)
            def _():
                two(i, 1).wait_send()
        @pl.loop(0, ns)
        def _(i):
            home(i).wait()
            back(i).wait()
        for i in (ns - 2, ns - 1):
            for k in range(2):
                keep(i, k).wait()
                give(i, k).wait_send()


def attention(q, do, kv, cos, sin, hd, heads=2, lag=2):
    batch, half_rows, width = q.shape
    ns, rows = batch // 2, 2 * half_rows
    mine = pl.BlockSpec((1, half_rows, heads * hd), lambda s, h: (lax.axis_index('sp') % 2 * ns + s, 0, h))
    tab = pl.BlockSpec((4 * rows, hd // 2), lambda s, h: (0, 0))
    hbm = pl.BlockSpec(memory_space=pl.ANY)
    act = jax.ShapeDtypeStruct(q.shape, BF16)
    dma = pltpu.SemaphoreType.DMA
    return pl.pallas_call(
        functools.partial(attn_kernel, heads, hd, lag),
        grid=(ns, width // (heads * hd)),
        in_specs=[mine, mine, hbm, hbm, hbm, tab, tab],
        out_specs=[hbm, hbm, hbm],
        out_shape=[act, act, jax.ShapeDtypeStruct(kv.shape, BF16)],
        scratch_shapes=[
            pltpu.VMEM((4, ns, rows, 2 * hd), BF16),
            pltpu.VMEM((4, rows, hd), BF16),
            pltpu.VMEM((ns, half_rows, width), BF16),
            pltpu.VMEM((ns, half_rows, width), BF16),
            pltpu.VMEM((2, 2, 2, half_rows, width), BF16),
            pltpu.VMEM((4, ns, rows, 2 * hd), F32),
            pltpu.VMEM((ns, rows, 2 * hd), F32),
            pltpu.VMEM((2, ns, rows, 2 * hd), F32),
            pltpu.VMEM((ns, rows, 2 * hd), BF16),
            dma, dma((2, 1)), dma((3, 2, ns)), dma((2, ns)), dma((2, 2, ns)), dma((2, 2)), dma((2, 2, ns)), dma((2, ns)), dma((2, 2, ns)), dma((ns,)), dma((2, ns)),
        ],
        compiler_params=pltpu.CompilerParams(dimension_semantics=("arbitrary", "arbitrary"), collective_id=2, has_side_effects=True, vmem_limit_bytes=66 * 1000 * 1000),
        cost_estimate=pl.CostEstimate(flops=6 * 2 * ns * rows * width * rows * 4, bytes_accessed=100 * 1024 * 1024, transcendentals=0),
        name="attention",
    )(q, do, q, do, kv, cos, sin)


def place_kernel(gwo, gwq, gwkv, a, d, wo, wq, wk, wv, a_out, d_out):
    hd = wk.shape[1]
    wo[...] = gwo[...]
    for h in range(wq.shape[1]):
        wq[:, h, :] = gwq[:, h * hd:(h + 1) * hd]
    t = gwkv[...].T
    wk[...] = t[:, :hd]
    wv[...] = t[:, hd:]
    a_out[...] = a[...]
    d_out[...] = d[...]


def place(gwo, gwq, gwkv, a, d, heads):
    m, n = gwq.shape
    hd = n // heads
    tile = 128
    rows = lambda w: pl.BlockSpec((tile, w), lambda i: (i, 0))
    return pl.pallas_call(
        place_kernel,
        grid=(m // tile,),
        in_specs=[rows(n), rows(n), pl.BlockSpec((2 * hd, tile), lambda i: (0, i)), rows(a.shape[1]), rows(d.shape[1])],
        out_specs=[rows(n), pl.BlockSpec((tile, heads, hd), lambda i: (i, 0, 0)), rows(hd), rows(hd), rows(a.shape[1]), rows(d.shape[1])],
        out_shape=[jax.ShapeDtypeStruct((m, n), F32), jax.ShapeDtypeStruct((m, heads, hd), F32), jax.ShapeDtypeStruct((m, hd), F32), jax.ShapeDtypeStruct((m, hd), F32), jax.ShapeDtypeStruct(a.shape, BF16), jax.ShapeDtypeStruct(d.shape, BF16)],
        compiler_params=pltpu.CompilerParams(dimension_semantics=("arbitrary",), vmem_limit_bytes=66 * 1000 * 1000),
        name="place",
    )(gwo, gwq, gwkv, a, d)


def solution(mesh):
    seq_spec = P(None, 'sp', None)
    rep_spec = P()

    def local_step(hidden, d_out, w_query, w_key, w_value, w_out):
        batch, local_len, width = hidden.shape
        hd = w_key.shape[1]
        qw = w_query.shape[1] * hd
        dev = lax.axis_index('sp')
        wo = w_out.reshape(qw, width)
        wq, wkv = lax.optimization_barrier((w_query.reshape(width, qw), jnp.concatenate([w_key, w_value], axis=1)))

        offset = jnp.arange(local_len)
        positions = [((dev ^ (2 * b)) ^ c) * local_len + offset for b in range(4) for c in range(2)]
        cos, sin = rope_tables(jnp.concatenate(positions), hd)

        proj = lambda x, w, eq: jnp.einsum(eq, x, w, preferred_element_type=F32).astype(BF16)
        kv = proj(hidden, wkv, 'bld,de->ble')
        do = proj(d_out, wo, 'bld,ed->ble')
        q = proj(hidden, wq, 'bld,de->ble')
        o, dq, dkv = attention(q, do, kv, cos, sin, hd)

        flat = lambda x: x.reshape(batch * local_len, -1)
        grad_wo, grad_wq, grad_wkv, attn_out, d_hidden = sum_all(flat(hidden), flat(d_out), flat(o), wo, flat(dq), wq, flat(dkv), wkv)
        grad_wo, grad_wq, grad_wk, grad_wv, attn_out, d_hidden = place(grad_wo, grad_wq, grad_wkv, attn_out, d_hidden, w_query.shape[1])
        return (attn_out.reshape(hidden.shape), d_hidden.reshape(hidden.shape), grad_wq, grad_wk, grad_wv, grad_wo.reshape(w_out.shape))

    return jax.shard_map(local_step, mesh=mesh, in_specs=(seq_spec, seq_spec, rep_spec, rep_spec, rep_spec, rep_spec), out_specs=(seq_spec, seq_spec, rep_spec, rep_spec, rep_spec, rep_spec), check_vma=False)
```
